32 devices in a mesh: dom: 4 (over y, core), rep: 8 (over z, x).
Axes of the slice: x: 2, y: 2, z: 4, core: 2. Of those that a mesh axis runs over, the one named last changes fastest.
Arguments:
- facts: float32 [131072, 256], P(('dom', 'rep')), may hold values from -6 to 6
- row_owner: int32 [131072, 1], P(('dom', 'rep')), may hold values from 0 to 3; in each aligned block of 4096 rows (0 to 4095, 4096 to 8191, ...) at most 2048 rows name the same one
- key_offset: int32 [131072], P(('dom', 'rep')), may hold values from 0 to 1023
Outputs:
- key_means: float32 [4096, 256], P(('dom', 'rep'))
- key_counts: float32 [4096], P(('dom', 'rep'))
The draws below stay inside these ranges and needn't reach their ends.
Inputs may be any that keep to these rules, and one draw needn't show every extreme that they name: `row_owner`: in the rows of one device no key range is named by more than 2048 rows, a bound that some block reaches.
All inputs are finite; a program needn't handle non-finite values.
Results may differ from the reference program's by a relative error of at most 0.0003.
Values sent between devices are 32-bit elements; how exact they have to be, the bound alone decides.
A program may use at most 64 MiB of HBM per device.

```python
import math
import jax
import jax.numpy as jnp
import numpy as np

M = 256
KEYS = 4096
ROWS_DEV = 4096
ROWS = 131072
RANGE = 1024
CAP = 2048
N_DOM = 4


def draw_key_offset(key, part):
    order_key = jax.random.fold_in(key, 11)
    kept_key = jax.random.fold_in(key, 12)
    first_key = jax.random.fold_in(key, 13)
    second_key = jax.random.fold_in(key, 14)
    inner_offsets = (jax.random.permutation(order_key, RANGE - 2) + 1).astype(jnp.int32)
    end_offsets = jnp.array([0, RANGE - 1], jnp.int32)
    kept_offsets = jnp.concatenate([end_offsets, inner_offsets[4:]])
    kept_offsets = jax.random.permutation(kept_key, kept_offsets).astype(jnp.int32)
    first_draw = jax.random.randint(first_key, (ROWS,), 0, RANGE - 4, dtype=jnp.int32)
    second_draw = jax.random.randint(second_key, (ROWS,), 0, RANGE - 4, dtype=jnp.int32)
    return kept_offsets[jnp.minimum(first_draw, second_draw)].astype(jnp.int32)


def block_levels(rng, shape, shards, least, top_value):
    factor_of = 1.0
    for axis_at, parts in shards:
        steps = jax.random.uniform(jax.random.fold_in(jax.random.fold_in(rng, 6), axis_at), (parts,), jnp.float32, least / len(shards), top_value / len(shards))
        factor_of = factor_of * jnp.repeat(jnp.exp(steps), shape[axis_at] // parts).reshape((-1,) + (1,) * (len(shape) - 1 - axis_at))
    return factor_of


def shared_out(stream_key, own, number, rows, amount, top, reach, skew):
    order = jax.random.permutation(stream_key, amount)
    packed, usual = shares(amount, rows * top, reach, skew, True), shares(amount, rows * top, reach, skew, False)
    places = jnp.arange(amount)

    def named(tallies, rotation):
        used = int((tallies > 0).sum())
        fixed = max(1, used // 4)
        shifted = fixed + (places - fixed + rotation * (used - fixed)) % max(1, amount - fixed)
        return jnp.zeros((amount,), jnp.int32).at[order[jnp.where(places < fixed, places, shifted)]].set(jnp.asarray(tallies, jnp.int32))

    tallies = jnp.where(number % 4 == 0, named(packed, number // 4), named(usual, number - number // 4 - 1))
    mixed = jax.random.permutation(jax.random.fold_in(own, 3), amount)
    source_of, taker = mixed[0:amount // 2 * 2:2], mixed[1:amount // 2 * 2:2]
    slack = jnp.minimum(tallies[source_of] - 1, reach - tallies[taker]) // 2
    slack = jnp.where((source_of == order[0]) | (taker == order[0]) | (tallies[taker] == 0), 0, jnp.maximum(slack, 0))
    shifted = jax.random.randint(jax.random.fold_in(own, 4), (amount // 2,), 0, 1 << 20) % (slack + 1)
    tallies = tallies.at[source_of].add(-shifted).at[taker].add(shifted)
    items = jnp.searchsorted(jnp.cumsum(tallies), jnp.arange(rows * top), side="right").astype(jnp.int32)
    grid = items.reshape(top, rows).T
    grid = grid[jax.random.permutation(jax.random.fold_in(own, 1), rows)]
    rotation = jax.random.randint(jax.random.fold_in(own, 2), (rows, 1), 0, top)
    return jnp.take_along_axis(grid, (jnp.arange(top)[None, :] + rotation) % top, axis=1)


def shares(count, total, most, slope, full):
    portions = [(1 << 20) // math.isqrt(grade ** slope) + 1 for grade in range(1, count + 1)]
    largest = most if full else min(most, max(-(-total // count), total * portions[0] // sum(portions)))
    least = 1 if total - largest >= count - 1 else 0
    holding, rest = [largest] + [least] * (count - 1), total - largest - least * (count - 1)
    while rest > 0:
        free = [i for i in range(1, count) if holding[i] < largest] or [i for i in range(1, count) if holding[i] < most]
        mass, remaining = sum([portions[i] for i in free]), rest
        for i in free:
            more = min(most - holding[i], max(1, remaining * portions[i] // mass), rest)
            holding[i] = holding[i] + more
            rest = rest - more
    return np.array(holding)


def centred(own_key, extent, deviation, bound, split=(), held_as=jnp.bfloat16):
    result = deviation * jax.random.normal(own_key, extent, jnp.float32)
    if split:
        result = result * block_levels(own_key, extent, split, -0.22, 0.18)
    return jnp.clip(result, -bound, bound).astype(held_as)


def setup_inputs(seed: int = 0) -> dict:
    splits = jax.random.split(jax.random.key(seed), 4)
    facts = centred(splits[0], (ROWS, M), 1.0, 6.0, ((0, 32),), jnp.float32)
    row_owner_keys = jax.random.split(jax.random.fold_in(splits[1], 1), ROWS // ROWS_DEV)
    row_owner_turns = jax.random.permutation(jax.random.fold_in(splits[1], 3), ROWS // ROWS_DEV)
    row_owner = jax.vmap(lambda own, number: shared_out(jax.random.fold_in(splits[1], 2), own, number, ROWS_DEV, N_DOM, 1, CAP, 2))(row_owner_keys, row_owner_turns).reshape((ROWS, 1))
    key_offset = draw_key_offset(jax.random.fold_in(splits[3], 71), 0)
    return dict(facts=facts, row_owner=row_owner, key_offset=key_offset)


def reference(facts, row_owner, key_offset):
    key_ids = row_owner[:, 0] * (KEYS // N_DOM) + key_offset
    key_sums = jax.ops.segment_sum(facts, key_ids, num_segments=KEYS)
    key_counts = jax.ops.segment_sum(jnp.ones(key_ids.shape, jnp.float32), key_ids, num_segments=KEYS)
    key_means = key_sums / jnp.maximum(key_counts, 1.0)[:, None]
    return key_means, key_counts
```

```python
import functools

import jax
import jax.numpy as jnp
from jax import lax
from jax.experimental import pallas as pl
from jax.experimental.pallas import tpu as pltpu
from jax.sharding import PartitionSpec as P

KEYS = 4096
MESH = pl.DeviceIdType.MESH
F32 = jnp.float32
BF16 = jnp.bfloat16
LANES = 128
TABLES = 4


def flip(index, bits):
    at = 1
    while at <= bits:
        if bits & at:
            index = index + at * (1 - 2 * ((index // at) % 2))
        at *= 2
    return index


def table_rows(D, Z, hb, me_d, me_r, owner, offset):
    kpd = 2 * hb
    rel = owner ^ me_d
    dc, d = rel & 1, rel >> 1
    i = offset & (kpd - 1)
    rr = (offset >> (kpd.bit_length() - 1)) ^ me_r
    x, z = rr & 1, rr >> 1
    blk_a = jnp.where(d > 0, 2 * (d - 1) + x, jnp.where(x > 0, 3 * D - 2, 4 * D - 2))
    blk_b = jnp.where(x > 0, 2 * (D - 1) + d, jnp.where(d > 0, 3 * D - 2 + d, 4 * D - 1))
    blk = jnp.where(i >= hb, blk_b, blk_a)
    lab = (((Z - 1 - z) * 2 + dc) * (4 * D) + blk) * hb + (i & (hb - 1))
    crow = ((dc * D + d) * 2 + x) * Z + z
    return lab, crow, i


def scatter(D, Z, hb, rows, owner_hbm, offset_hbm, facts_hbm, *refs):
    tabs, refs = refs[:TABLES], refs[TABLES:]
    owner_ref, offset_ref, lab_ref, at_ref, fbuf, isem, lsem, fsem = refs
    me_d, me_r = lax.axis_index("dom"), lax.axis_index("rep")
    nchunks = fsem.shape[0]
    words = 2 * rows // nchunks
    loads = [
        pltpu.make_async_copy(
            facts_hbm.at[pl.ds(k * words, words)], fbuf.at[pl.ds(k * words, words)], fsem.at[k]
        )
        for k in range(nchunks)
    ]
    ints = [
        pltpu.make_async_copy(owner_hbm, owner_ref, isem.at[0]),
        pltpu.make_async_copy(offset_hbm, offset_ref, isem.at[1]),
    ]
    for ld in ints + loads:
        ld.start()
    for ld in ints:
        ld.wait()
    lab_ref[...] = 2 * table_rows(D, Z, hb, me_d, me_r, owner_ref[...], offset_ref[...])[0]
    labels = pltpu.make_async_copy(lab_ref, at_ref, lsem)
    labels.start()

    @pl.loop(0, 2 * KEYS // 128)
    def _(i):
        at = pl.ds(pl.multiple_of(i * 128, 128), 128)
        for tab in tabs:
            tab[at, :] = jnp.zeros((128, LANES), F32)

    labels.wait()
    group = rows // nchunks // LANES
    for k in range(nchunks):
        loads[k].wait()

        @pl.loop(0, group)
        def _(g):
            base = pl.multiple_of((k * group + g) * 2 * LANES, 2 * LANES)
            for r in range(0, LANES, TABLES):
                at = [pl.multiple_of(at_ref[k * group + g, r + u], 2) for u in range(TABLES)]
                row = [fbuf[pl.ds(base + 16 * ((r + u) // 8) + (r + u) % 8, 2, stride=8), :] for u in range(TABLES)]
                row = [tabs[u][pl.ds(at[u], 2), :] + row[u] for u in range(TABLES)]
                for u in range(TABLES):
                    tabs[u][pl.ds(at[u], 2), :] = row[u]


def kernel(D, Z, hb, rows, owner_hbm, offset_hbm, *refs):
    tabs, refs = refs[:TABLES], refs[TABLES:]
    (out_ref, cout_ref, owner_ref, offset_ref, tab, recvC1, recvC2,
     rA1, rB1, rA2, rB2, rZ,
     c0, cS, cR, cD, cX, cXr, cZ, cZr, isem,
     sC1, tC1, sC2, tC2, sA1, tA1, sB1, tB1, sA2, tA2, sB2, tB2, sZ, tZ,
     scC, tcC, scD, tcD, scX, tcX, scZ, tcZ) = refs
    me_d, me_r = lax.axis_index("dom"), lax.axis_index("rep")
    kpd = 2 * hb
    hb = 2 * hb
    T1, T2 = (3 * D - 2) * hb, (D + 2) * hb
    stage = 4 * D * hb
    core = (flip(me_d, 1), me_r)
    dpeer = [None] + [(flip(me_d, 2 * d), me_r) for d in range(1, D)]
    xpeer = (me_d, flip(me_r, 1))
    zpeer = [None] + [(me_d, flip(me_r, 2 * z)) for z in range(1, Z)]
    peers = [core] + dpeer[1:] + [xpeer] + zpeer[1:]

    ints = [
        pltpu.make_async_copy(owner_hbm, owner_ref, isem.at[0]),
        pltpu.make_async_copy(offset_hbm, offset_ref, isem.at[1]),
    ]
    for ld in ints:
        ld.start()
    barrier = pltpu.get_barrier_semaphore()
    for p in peers:
        pl.semaphore_signal(barrier, inc=1, device_id=p, device_id_type=MESH)

    def rcopy(src, dst, s, t, dev):
        return pltpu.make_async_remote_copy(
            src_ref=src, dst_ref=dst, send_sem=s, recv_sem=t, device_id=dev, device_id_type=MESH
        )

    def tile(t):
        i, j = t // 4, t % 4
        start = (2 * i + 1 - j % 2) * stage + (j // 2) * T1
        size = max(T1, T2)
        step = min(size, 128)

        @pl.loop(0, size // step)
        def _(n):
            at = pl.ds(pl.multiple_of(start + n * step, 8), step)
            v = tabs[0][at, :]
            for other in tabs[1:]:
                v = v + other[at, :]
            tab[t, pl.ds(pl.multiple_of(n * step, 8), step), :] = v

    def counts():
        for ld in ints:
            ld.wait()
        nrow = 4 * D * Z
        _, crow, i = table_rows(D, Z, kpd // 2, me_d, me_r, owner_ref[...], offset_ref[...])
        hot_r = jnp.where(lax.broadcasted_iota(jnp.int32, (nrow, rows), 0) == crow, 1.0, 0.0).astype(BF16)
        hot_c = jnp.where(lax.broadcasted_iota(jnp.int32, (kpd, rows), 0) == i, 1.0, 0.0).astype(BF16)
        cnt = lax.dot_general(hot_r, hot_c, (((1,), (1,)), ((), ())), preferred_element_type=F32)
        half = nrow // 2
        for d in range(D):
            c0[d] = cnt[d * 2 * Z:(d + 1) * 2 * Z]
            cS[d] = cnt[half + d * 2 * Z:half + (d + 1) * 2 * Z]
        cc.start()

    cc = rcopy(cS, cR, scC, tcC, core)

    def C1(i):
        return rcopy(tab.at[4 * i, pl.ds(0, T1)], recvC1.at[i], sC1.at[i], tC1.at[i], core)

    def C2(i):
        return rcopy(tab.at[4 * i + 2, pl.ds(0, T2)], recvC2.at[i], sC2.at[i], tC2.at[i], core)

    def A1(i, d):
        return rcopy(tab.at[4 * i + 1, pl.ds(2 * (d - 1) * hb, 2 * hb)], rA1.at[i, d - 1],
                     sA1.at[i, d - 1], tA1.at[i, d - 1], dpeer[d])

    def B1(i):
        return rcopy(tab.at[4 * i + 1, pl.ds(2 * (D - 1) * hb, D * hb)], rB1.at[i], sB1.at[i], tB1.at[i], xpeer)

    def A2(i):
        return rcopy(tab.at[4 * i + 3, pl.ds(0, hb)], rA2.at[i], sA2.at[i], tA2.at[i], xpeer)

    def B2(i, d):
        return rcopy(tab.at[4 * i + 3, pl.ds(d * hb, hb)], rB2.at[i, d - 1], sB2.at[i, d - 1], tB2.at[i, d - 1], dpeer[d])

    def ZC(i, z):
        return rcopy(tab.at[4 * i + 3, pl.ds(D * hb, 2 * hb)], rZ.at[i], sZ.at[i], tZ.at[i], zpeer[z])

    def phase1(i):
        C1(i).wait_recv()
        tab[4 * i + 1, 0:T1] = tab[4 * i + 1, 0:T1] + recvC1[i]
        for d in range(1, D):
            A1(i, d).start()
        B1(i).start()

    def core2(i):
        C2(i).wait_recv()
        tab[4 * i + 3, 0:T2] = tab[4 * i + 3, 0:T2] + recvC2[i]

    def phase2(i):
        x0 = pl.ds(D * hb, hb)
        for d in range(1, D):
            A1(i, d).wait_recv()
            tab[4 * i + 3, 0:hb] = tab[4 * i + 3, 0:hb] + rA1[i, d - 1, hb:2 * hb]
        A2(i).start()
        B1(i).wait_recv()
        for d in range(1, D):
            tab[4 * i + 3, d * hb:(d + 1) * hb] = tab[4 * i + 3, d * hb:(d + 1) * hb] + rB1[i, d * hb:(d + 1) * hb]
            B2(i, d).start()
        extra = rA1[i, 0, 0:hb]
        for d in range(2, D):
            extra = extra + rA1[i, d - 1, 0:hb]
        tab[4 * i + 3, x0] = tab[4 * i + 3, x0] + extra
        b0 = pl.ds((D + 1) * hb, hb)
        tab[4 * i + 3, b0] = tab[4 * i + 3, b0] + rB1[i, 0:hb]

    def phase3(i):
        x0 = pl.ds(D * hb, hb)
        b0 = pl.ds((D + 1) * hb, hb)
        A2(i).wait_recv()
        tab[4 * i + 3, x0] = tab[4 * i + 3, x0] + rA2[i]
        for d in range(1, D):
            B2(i, d).wait_recv()
            tab[4 * i + 3, b0] = tab[4 * i + 3, b0] + rB2[i, d - 1]
        for z in range(1, Z):
            if isinstance(i, int):
                if i == Z - 1 - z:
                    ZC(i, z).start()
                continue

            @pl.when(i == Z - 1 - z)
            def _():
                ZC(i, z).start()

    def DC(d):
        return rcopy(c0.at[d], cD.at[d - 1], scD.at[d - 1], tcD.at[d - 1], dpeer[d])

    def XC():
        return rcopy(cX, cXr, scX, tcX, xpeer)

    def ZCc(z):
        return rcopy(cZ, cZr.at[z - 1], scZ.at[z - 1], tcZ.at[z - 1], zpeer[z])

    def count_step(i):
        @pl.when(i == 0)
        def _():
            cc.wait_recv()
            for d in range(D):
                c0[d] = c0[d] + cR[d]
            for d in range(1, D):
                DC(d).start()

        @pl.when(i == 1)
        def _():
            v = c0[0]
            for d in range(1, D):
                DC(d).wait_recv()
                v = v + cD[d - 1]
            cX[...] = v
            XC().start()

        @pl.when(i == 2)
        def _():
            XC().wait_recv()
            cZ[...] = cX[0:Z] + cXr[Z:2 * Z]
            for z in range(1, Z):
                ZCc(z).start()

    tile(0)
    pl.semaphore_wait(barrier, len(peers))
    C1(0).start()
    counts()

    @pl.loop(1, 4 * Z)
    def _(t):
        i, j = t // 4, t % 4
        tile(t)

        @pl.when(j == 0)
        def _():
            C1(i).start()
            core2(i - 1)

        @pl.when(j == 1)
        def _():
            phase1(i)
            count_step(i)

        @pl.when(j == 2)
        def _():
            C2(i).start()

        @pl.when((j == 2) & (i >= 1))
        def _():
            phase2(i - 1)

        @pl.when((j == 3) & (i >= 2))
        def _():
            phase3(i - 2)

    core2(Z - 1)
    phase2(Z - 1)
    phase3(Z - 2)
    phase3(Z - 1)
    cf = cZ[0:1, :]
    for z in range(1, Z):
        ZCc(z).wait_recv()
        cf = cf + cZr[z - 1, z:z + 1, :]
    cout_ref[...] = cf
    spread = jnp.broadcast_to(jnp.maximum(cf, 1.0), (kpd, kpd))
    eye = lax.broadcasted_iota(jnp.int32, (kpd, kpd), 0) == lax.broadcasted_iota(jnp.int32, (kpd, kpd), 1)
    col = jnp.sum(jnp.where(eye, spread, 0.0), axis=1, keepdims=True)
    tot = tab[4 * Z - 1, D * hb:(D + 2) * hb]
    for i in range(Z - 1):
        ZC(i, Z - 1 - i).wait_recv()
        tot = tot + rZ[i]
    rZ[Z - 1] = tot
    last = rZ.at[Z - 1]
    out_ref[:, 0:LANES] = last[pl.ds(0, kpd, stride=2), :] / col
    out_ref[:, LANES:2 * LANES] = last[pl.ds(1, kpd, stride=2), :] / col

    cc.wait_send()
    for d in range(1, D):
        DC(d).wait_send()
    XC().wait_send()
    for z in range(1, Z):
        ZCc(z).wait_send()
        ZC(Z - 1 - z, z).wait_send()

    @pl.loop(0, Z)
    def _(i):
        C1(i).wait_send()
        C2(i).wait_send()
        for d in range(1, D):
            A1(i, d).wait_send()
            B2(i, d).wait_send()
        B1(i).wait_send()
        A2(i).wait_send()


def per_device(facts, row_owner, key_offset):
    n_dom, n_rep = lax.axis_size("dom"), lax.axis_size("rep")
    rows, M = facts.shape
    D, Z = n_dom // 2, n_rep // 2
    kpd = KEYS // (n_dom * n_rep)
    hb = kpd // 2
    T1, T2 = 2 * (3 * D - 2) * hb, 2 * (D + 2) * hb
    nchunks = 2

    def vm(*shape, dtype=F32):
        return pltpu.VMEM(shape, dtype)

    def dma(*shape):
        return [pltpu.SemaphoreType.DMA(shape)] * 2 if shape else [pltpu.SemaphoreType.DMA] * 2

    I32 = jnp.int32
    pin = pltpu.with_memory_space_constraint
    hbm = pl.BlockSpec(memory_space=pltpu.HBM)
    vmem = pl.BlockSpec(memory_space=pltpu.VMEM)
    by_tile = facts.reshape(rows // 8, 8, 2, LANES).transpose(0, 2, 1, 3).reshape(2 * rows, LANES)
    square = (rows // LANES, LANES)
    tables = pl.pallas_call(
        functools.partial(scatter, D, Z, hb, rows),
        out_shape=[vm(2 * KEYS, LANES)] * TABLES,
        in_specs=[hbm] * 3,
        out_specs=[vmem] * TABLES,
        scratch_shapes=[
            vm(*square, dtype=I32), vm(*square, dtype=I32), vm(*square, dtype=I32), pltpu.SMEM(square, I32),
            vm(2 * rows, LANES),
            pltpu.SemaphoreType.DMA((2,)), pltpu.SemaphoreType.DMA, pltpu.SemaphoreType.DMA((nchunks,)),
        ],
        compiler_params=pltpu.CompilerParams(vmem_limit_bytes=24 * 1024 * 1024),
    )(*(pin(a, pltpu.HBM) for a in (row_owner.reshape(square), key_offset.reshape(square), by_tile)))

    h = 2 * hb
    scratch = [
        vm(1, rows, dtype=I32), vm(1, rows, dtype=I32),
        vm(4 * Z, max(T1, T2), LANES), vm(Z, T1, LANES), vm(Z, T2, LANES),
        vm(Z, D - 1, 2 * h, LANES), vm(Z, D * h, LANES), vm(Z, h, LANES), vm(Z, D - 1, h, LANES), vm(Z, 2 * h, LANES),
        vm(D, 2 * Z, kpd), vm(D, 2 * Z, kpd), vm(D, 2 * Z, kpd), vm(D - 1, 2 * Z, kpd),
        vm(2 * Z, kpd), vm(2 * Z, kpd), vm(Z, kpd), vm(Z - 1, Z, kpd),
        pltpu.SemaphoreType.DMA((2,)),
        *dma(Z), *dma(Z), *dma(Z, D - 1), *dma(Z), *dma(Z), *dma(Z, D - 1), *dma(Z - 1),
        *dma(), *dma(D - 1), *dma(), *dma(Z - 1),
    ]
    means, counts = pl.pallas_call(
        functools.partial(kernel, D, Z, hb, rows),
        out_shape=(jax.ShapeDtypeStruct((kpd, M), F32), jax.ShapeDtypeStruct((1, kpd), F32)),
        in_specs=[hbm] * 2 + [vmem] * TABLES,
        out_specs=(vmem, vmem),
        scratch_shapes=scratch,
        compiler_params=pltpu.CompilerParams(
            collective_id=0, has_side_effects=True, vmem_limit_bytes=24 * 1024 * 1024
        ),
    )(
        pin(row_owner.reshape(1, rows), pltpu.HBM), pin(key_offset.reshape(1, rows), pltpu.HBM),
        *(pin(table, pltpu.VMEM) for table in tables),
    )
    return means, counts.reshape(kpd)


def solution(mesh):
    placed = (P(("dom", "rep"), None), P(("dom", "rep"), None), P(("dom", "rep")))
    return jax.shard_map(
        per_device,
        mesh=mesh,
        in_specs=placed,
        out_specs=(P(("dom", "rep"), None), P(("dom", "rep"))),
        check_vma=False,
    )
```

```python
import functools

import jax
import jax.numpy as jnp
from jax import lax
from jax.experimental import pallas as pl
from jax.experimental.pallas import tpu as pltpu
from jax.sharding import PartitionSpec as P

KEYS = 4096
MESH = pl.DeviceIdType.MESH
F32 = jnp.float32
BF16 = jnp.bfloat16
LANES = 128
TABLES = 4
PAIR = 2
SIDE = 28


def flip(index, bits):
    at = 1
    while at <= bits:
        if bits & at:
            index = index + at * (1 - 2 * ((index // at) % 2))
        at *= 2
    return index


def log2(n):
    return n.bit_length() - 1


def routes(n_dom, n_rep, kpd):
    x, y = (0, 1), (2, 0)
    rest = [(1 << b, 0) for b in range(2, log2(n_dom))] + [(0, 1 << b) for b in range(1, log2(n_rep))]
    side = kpd * SIDE // 128 // 4 * 4
    parts = [(0, kpd - side, ([x, y, *rest], [y, x, *rest]))]
    if side:
        parts.append((kpd - side, side, ([*rest, y, x], [*rest, x, y])))
    return parts


def label(orders, n_dom, n_rep, me_d, me_r, owner, rep):
    rel_d, rel_r = owner ^ me_d, rep ^ me_r
    found = []
    for order in orders:
        r = rel_d & 1
        for bit_d, bit_r in order:
            bit = rel_d >> log2(bit_d) if bit_d else rel_r >> log2(bit_r)
            r = 2 * r + (bit & 1)
        found.append(r)
    return jnp.where((owner & 1) == 0, found[0], found[1])


def scatter(parts, n_dom, n_rep, rows, owner_hbm, offset_hbm, owner_row_hbm, offset_row_hbm, facts_hbm, *refs):
    tabs, refs = refs[:TABLES], refs[TABLES:]
    cnt_ref, owner_ref, offset_ref, owner_row, offset_row, lab_ref, at_ref, fbuf, isem, lsem, fsem = refs
    me_d, me_r = lax.axis_index("dom"), lax.axis_index("rep")
    blocks = n_dom * n_rep // 2
    kpd = KEYS // (2 * blocks)
    nchunks = fsem.shape[0]
    words = 2 * rows // nchunks
    ints = [
        pltpu.make_async_copy(src, dst, isem.at[k])
        for k, (src, dst) in enumerate(
            [(owner_hbm, owner_ref), (offset_hbm, offset_ref), (owner_row_hbm, owner_row), (offset_row_hbm, offset_row)]
        )
    ]
    loads = [
        pltpu.make_async_copy(
            facts_hbm.at[pl.ds(k * words, words)], fbuf.at[pl.ds(k * words, words)], fsem.at[k]
        )
        for k in range(nchunks)
    ]
    for ld in ints + loads:
        ld.start()

    def clear(first, last):
        @pl.loop(0, KEYS // 64)
        def _(i):
            at = pl.ds(pl.multiple_of(i * 128, 128), 128)
            for tab in tabs[first:last]:
                tab[at, :] = jnp.zeros((128, LANES), F32)

    clear(0, TABLES // 2)
    for ld in ints[:2]:
        ld.wait()
    owner, offset = owner_ref[...], offset_ref[...]
    i, base, word = offset & (kpd - 1), 0, None
    for first, keys, orders in parts:
        r = label(orders, n_dom, n_rep, me_d, me_r, owner, offset >> log2(kpd))
        at = base + 2 * (r * keys + i - first)
        word = at if word is None else jnp.where(i >= first, at, word)
        base += 4 * blocks * keys
    lab_ref[...] = word
    labels = pltpu.make_async_copy(lab_ref, at_ref, lsem)
    labels.start()
    clear(TABLES // 2, TABLES)
    for ld in ints[2:]:
        ld.wait()
    owner, offset = owner_row[...], offset_row[...]
    r = label(parts[0][2], n_dom, n_rep, me_d, me_r, owner, offset >> log2(kpd))
    i = offset & (kpd - 1)
    hot_r = jnp.where(lax.broadcasted_iota(jnp.int32, (2 * blocks, rows), 0) == r, 1.0, 0.0).astype(BF16)
    hot_i = jnp.where(lax.broadcasted_iota(jnp.int32, (LANES, rows), 0) == i, 1.0, 0.0).astype(BF16)
    cnt_ref[...] = lax.dot_general(hot_r, hot_i, (((1,), (1,)), ((), ())), preferred_element_type=F32)

    labels.wait()
    group = rows // nchunks // LANES
    for k in range(nchunks):
        loads[k].wait()

        @pl.loop(0, group)
        def _(g):
            base = pl.multiple_of((k * group + g) * 2 * LANES, 2 * LANES)
            mine = at_ref.at[k * group + g]
            for r in range(0, LANES, TABLES * PAIR):
                at = [pl.multiple_of(mine[r + u], 2) for u in range(TABLES * PAIR)]
                row = [fbuf[pl.ds(base + 16 * ((r + u) // 8) + (r + u) % 8, 2, stride=8), :] for u in range(TABLES * PAIR)]
                old = [tabs[u % TABLES][pl.ds(at[u], 2), :] for u in range(TABLES * PAIR)]
                for u in range(TABLES):
                    old[u] = old[u] + row[u]
                    for v in range(u + TABLES, TABLES * PAIR, TABLES):
                        old[v] = jnp.where(at[v] == at[u], old[u], old[v]) + row[v]
                for u in range(TABLES * PAIR):
                    tabs[u % TABLES][pl.ds(at[u], 2), :] = old[u]


def kernel(parts, n_dom, n_rep, cnt_ref, *refs):
    blocks = n_dom * n_rep // 2
    kpd = KEYS // (n_dom * n_rep)
    depth = log2(blocks)
    tabs, (out_ref, cout_ref, final, *refs) = refs[:TABLES], refs[TABLES:]
    buffers = [refs[8 * q:8 * q + 8] for q in range(len(parts))]
    me_d, me_r = lax.axis_index("dom"), lax.axis_index("rep")
    c = me_d % 2
    core = (flip(me_d, 1), me_r)
    peers = [core] + [(flip(me_d, d), flip(me_r, r)) for d, r in parts[0][2][0]]
    barrier = pltpu.get_barrier_semaphore()
    for p in peers:
        pl.semaphore_signal(barrier, inc=1, device_id=p, device_id_type=MESH)

    def rcopy(src, dst, s, t, dev):
        return pltpu.make_async_remote_copy(
            src_ref=src, dst_ref=dst, send_sem=s, recv_sem=t, device_id=dev, device_id_type=MESH
        )

    def across(q, r):
        out, come, _, _, s, t, _, _ = buffers[q]
        return rcopy(out.at[r], come.at[r], s.at[r], t.at[r], core)

    def message(q, r, step):
        _, _, acc, got, _, _, s, t = buffers[q]
        (d0, r0), (d1, r1) = (order[step] for order in parts[q][2])
        peer = ((1 - c) * flip(me_d, d0) + c * flip(me_d, d1), (1 - c) * flip(me_r, r0) + c * flip(me_r, r1))
        return rcopy(acc.at[r], got.at[r], s.at[r], t.at[r], peer)

    bases = [4 * blocks * sum(p[1] for p in parts[:q]) for q in range(len(parts))]

    def local(q, other, r, put):
        words = 2 * parts[q][1]
        at = pl.ds(pl.multiple_of(bases[q] + (other * blocks + r) * words, 8), words)
        v = tabs[0][at, :]
        for tab in tabs[1:]:
            v = v + tab[at, :]
        put(slice(0, words), v)
        if q == 0:
            put(slice(words, words + 1), cnt_ref[pl.ds(other * blocks + r, 1), :])

    def total(q, r, step, put):
        _, come, _, got = buffers[q][:4]
        across(q, r).wait_recv()
        come_from = [come.at[r]]
        for k in range(step):
            at = r + (blocks >> (k + 1))
            message(q, at, k).wait_recv()
            come_from.append(got.at[at])

        def add(rows, v):
            for ref in come_from:
                v = v + ref[rows, :]
            put(rows, v)

        local(q, 0, r, add)

    def into(ref, r):
        def put(rows, v):
            ref[r, rows, :] = v
        return put

    pl.semaphore_wait(barrier, len(peers))

    @pl.loop(0, blocks)
    def _(n):
        for q in range(len(parts)):
            r = blocks - 1 - n
            local(q, 1, r, into(buffers[q][0], r))
            across(q, r).start()

    for step in range(depth):
        size = blocks >> (step + 1)

        @pl.loop(0, size)
        def _(n):
            for q in range(len(parts)):
                r = 2 * size - 1 - n
                total(q, r, step, into(buffers[q][2], r))
                message(q, r, step).start()

    for q in reversed(range(len(parts))):
        first, keys, _ = parts[q]

        def put(rows, v):
            if rows.start < 2 * keys:
                final[2 * first:2 * (first + keys), :] = v
            else:
                final[2 * kpd:2 * kpd + 1, :] = v

        total(q, 0, depth, put)
    cf = final[2 * kpd:2 * kpd + 1, 0:kpd]
    cout_ref[...] = cf
    spread = jnp.broadcast_to(jnp.maximum(cf, 1.0), (kpd, kpd))
    eye = lax.broadcasted_iota(jnp.int32, (kpd, kpd), 0) == lax.broadcasted_iota(jnp.int32, (kpd, kpd), 1)
    col = jnp.sum(jnp.where(eye, spread, 0.0), axis=1, keepdims=True)
    out_ref[:, 0:LANES] = final[pl.ds(0, kpd, stride=2), :] / col
    out_ref[:, LANES:2 * LANES] = final[pl.ds(1, kpd, stride=2), :] / col

    @pl.loop(0, blocks)
    def _(r):
        for q in range(len(parts)):
            across(q, r).wait_send()

    for step in range(depth):
        size = blocks >> (step + 1)

        @pl.loop(size, 2 * size)
        def _(r):
            for q in range(len(parts)):
                message(q, r, step).wait_send()


def per_device(facts, row_owner, key_offset):
    n_dom, n_rep = lax.axis_size("dom"), lax.axis_size("rep")
    rows, M = facts.shape
    blocks = n_dom * n_rep // 2
    kpd = KEYS // (n_dom * n_rep)
    parts = routes(n_dom, n_rep, kpd)
    nchunks = 2

    def vm(*shape, dtype=F32):
        return pltpu.VMEM(shape, dtype)

    def dma(*shape):
        return [pltpu.SemaphoreType.DMA(shape)] * 2 if shape else [pltpu.SemaphoreType.DMA] * 2

    I32 = jnp.int32
    pin = pltpu.with_memory_space_constraint
    hbm = pl.BlockSpec(memory_space=pltpu.HBM)
    vmem = pl.BlockSpec(memory_space=pltpu.VMEM)
    by_tile = facts.reshape(rows // 8, 8, 2, LANES).transpose(0, 2, 1, 3).reshape(2 * rows, LANES)
    square = (rows // LANES, LANES)
    ints = [row_owner.reshape(square), key_offset.reshape(square), row_owner.reshape(1, rows), key_offset.reshape(1, rows)]
    *tables, counted = pl.pallas_call(
        functools.partial(scatter, parts, n_dom, n_rep, rows),
        out_shape=[vm(2 * KEYS, LANES)] * TABLES + [vm(2 * blocks, LANES)],
        in_specs=[hbm] * 5,
        out_specs=[vmem] * (TABLES + 1),
        scratch_shapes=[
            vm(*square, dtype=I32), vm(*square, dtype=I32), vm(1, rows, dtype=I32), vm(1, rows, dtype=I32),
            vm(*square, dtype=I32), pltpu.SMEM(square, I32), vm(2 * rows, LANES),
            pltpu.SemaphoreType.DMA((4,)), pltpu.SemaphoreType.DMA, pltpu.SemaphoreType.DMA((nchunks,)),
        ],
        compiler_params=pltpu.CompilerParams(vmem_limit_bytes=24 * 1024 * 1024),
    )(*(pin(a, pltpu.HBM) for a in ints + [by_tile]))

    scratch = [vm(2 * kpd + 8, LANES)]
    for q, (_, keys, _) in enumerate(parts):
        scratch += [vm(blocks, 2 * keys + (q == 0), LANES)] * 4 + dma(blocks) + dma(blocks)
    means, counts = pl.pallas_call(
        functools.partial(kernel, parts, n_dom, n_rep),
        out_shape=(jax.ShapeDtypeStruct((kpd, M), F32), jax.ShapeDtypeStruct((1, kpd), F32)),
        in_specs=[vmem] * (TABLES + 1),
        out_specs=(vmem, vmem),
        scratch_shapes=scratch,
        compiler_params=pltpu.CompilerParams(
            collective_id=0, has_side_effects=True, vmem_limit_bytes=24 * 1024 * 1024
        ),
    )(*(pin(a, pltpu.VMEM) for a in (counted, *tables)))
    return means, counts.reshape(kpd)


def solution(mesh):
    placed = (P(("dom", "rep"), None), P(("dom", "rep"), None), P(("dom", "rep")))
    return jax.shard_map(
        per_device,
        mesh=mesh,
        in_specs=placed,
        out_specs=(P(("dom", "rep"), None), P(("dom", "rep"))),
        check_vma=False,
    )
```

```python
import functools

import jax
import jax.numpy as jnp
from jax import lax
from jax.experimental import pallas as pl
from jax.experimental.pallas import tpu as pltpu
from jax.sharding import PartitionSpec as P

KEYS = 4096
MESH = pl.DeviceIdType.MESH
F32 = jnp.float32
BF16 = jnp.bfloat16
LANES = 128
TABLES = 6
LAG = 8
TURNS = (
    31, 40, 15, 29, 30, 47, 45, 44, 27, 46, 23, 7, 41, 11, 39, 25,
    13, 37, 14, 43, 19, 26, 21, 3, 22, 36, 9, 38, 5, 6, 28, 17,
    42, 10, 12, 18, 24, 35, 8, 1, 20, 2, 34, 33, 4, 32, 16, 0,
)


def flip(index, bits):
    at = 1
    while at <= bits:
        if bits & at:
            index = index + at * (1 - 2 * ((index // at) % 2))
        at *= 2
    return index


def log2(n):
    return n.bit_length() - 1


def routes(n_dom, n_rep, kpd):
    x, y = (0, 1), (2, 0)
    rest = [(1 << b, 0) for b in range(2, log2(n_dom))] + [(0, 1 << b) for b in range(1, log2(n_rep))]
    flat, tall = ([x, y, *rest], [y, x, *rest]), ([*rest, y, x], [*rest, x, y])
    cuts = [kpd * at // 128 // 4 * 4 for at in (0, 52, 100)] + [kpd]
    ways = [flat, flat, tall]
    return [(cuts[q], cuts[q + 1] - cuts[q], way) for q, way in enumerate(ways) if cuts[q] < cuts[q + 1]]


def turns(blocks, parts):
    if blocks == 16 and len(parts) == 3:
        return [divmod(turn, 16) for turn in TURNS]
    return [(q, r) for r in reversed(range(blocks)) for q in range(len(parts))]


def label(orders, n_dom, n_rep, me_d, me_r, owner, rep):
    rel_d, rel_r = owner ^ me_d, rep ^ me_r
    found = []
    for order in orders:
        r = rel_d & 1
        for bit_d, bit_r in order:
            bit = rel_d >> log2(bit_d) if bit_d else rel_r >> log2(bit_r)
            r = 2 * r + (bit & 1)
        found.append(r)
    return jnp.where((owner & 1) == 0, found[0], found[1])


def scatter(parts, n_dom, n_rep, rows, owner_hbm, offset_hbm, owner_row_hbm, offset_row_hbm, facts_hbm, *refs):
    tabs, refs = refs[:TABLES], refs[TABLES:]
    cnt_ref, owner_ref, offset_ref, owner_row, offset_row, lab_ref, at_ref, fbuf, isem, lsem, fsem = refs
    me_d, me_r = lax.axis_index("dom"), lax.axis_index("rep")
    blocks = n_dom * n_rep // 2
    kpd = KEYS // (2 * blocks)
    nchunks = fsem.shape[0]
    words = 2 * rows // nchunks
    ints = [
        pltpu.make_async_copy(src, dst, isem.at[k])
        for k, (src, dst) in enumerate(
            [(owner_hbm, owner_ref), (offset_hbm, offset_ref), (owner_row_hbm, owner_row), (offset_row_hbm, offset_row)]
        )
    ]
    loads = [
        pltpu.make_async_copy(
            facts_hbm.at[pl.ds(k * words, words)], fbuf.at[pl.ds(k * words, words)], fsem.at[k]
        )
        for k in range(nchunks)
    ]
    for ld in ints + loads:
        ld.start()

    def clear(first, last):
        @pl.loop(0, KEYS // 64)
        def _(i):
            at = pl.ds(pl.multiple_of(i * 128, 128), 128)
            for tab in tabs[first:last]:
                tab[at, :] = jnp.zeros((128, LANES), F32)

    clear(0, TABLES // 2)
    for ld in ints[:2]:
        ld.wait()
    owner, offset = owner_ref[...], offset_ref[...]
    i, base, word = offset & (kpd - 1), 0, None
    for first, keys, orders in parts:
        r = label(orders, n_dom, n_rep, me_d, me_r, owner, offset >> log2(kpd))
        at = base + 2 * (r * keys + i - first)
        word = at if word is None else jnp.where(i >= first, at, word)
        base += 4 * blocks * keys
    lab_ref[...] = word
    labels = pltpu.make_async_copy(lab_ref, at_ref, lsem)
    labels.start()
    clear(TABLES // 2, TABLES)
    for ld in ints[2:]:
        ld.wait()
    owner, offset = owner_row[...], offset_row[...]
    r = label(parts[0][2], n_dom, n_rep, me_d, me_r, owner, offset >> log2(kpd))
    i = offset & (kpd - 1)
    hot_r = jnp.where(lax.broadcasted_iota(jnp.int32, (2 * blocks, rows), 0) == r, 1.0, 0.0).astype(BF16)
    hot_i = jnp.where(lax.broadcasted_iota(jnp.int32, (LANES, rows), 0) == i, 1.0, 0.0).astype(BF16)
    cnt_ref[...] = lax.dot_general(hot_r, hot_i, (((1,), (1,)), ((), ())), preferred_element_type=F32)

    labels.wait()
    group = rows // nchunks // LANES
    for k in range(nchunks):
        loads[k].wait()

        @pl.loop(0, group)
        def _(g):
            base = pl.multiple_of((k * group + g) * 2 * LANES, 2 * LANES)
            mine = at_ref.at[k * group + g]
            for r in range(LANES):
                at = pl.ds(pl.multiple_of(mine[r], 2), 2)
                row = fbuf[pl.ds(base + 16 * (r // 8) + r % 8, 2, stride=8), :]
                tabs[r % TABLES][at, :] = tabs[r % TABLES][at, :] + row


def kernel(parts, n_dom, n_rep, cnt_ref, *refs):
    blocks = n_dom * n_rep // 2
    kpd = KEYS // (n_dom * n_rep)
    depth = log2(blocks)
    tabs, (out_ref, cout_ref, final, *refs) = refs[:TABLES], refs[TABLES:]
    buffers = [refs[8 * q:8 * q + 8] for q in range(len(parts))]
    me_d, me_r = lax.axis_index("dom"), lax.axis_index("rep")
    c = me_d % 2
    core = (flip(me_d, 1), me_r)
    peers = [core] + [(flip(me_d, d), flip(me_r, r)) for d, r in parts[0][2][0]]
    barrier = pltpu.get_barrier_semaphore()
    for p in peers:
        pl.semaphore_signal(barrier, inc=1, device_id=p, device_id_type=MESH)

    def rcopy(src, dst, s, t, dev):
        return pltpu.make_async_remote_copy(
            src_ref=src, dst_ref=dst, send_sem=s, recv_sem=t, device_id=dev, device_id_type=MESH
        )

    def across(q, r):
        out, come, _, _, s, t, _, _ = buffers[q]
        return rcopy(out.at[r], come.at[r], s.at[r], t.at[r], core)

    def message(q, r, step):
        _, _, acc, got, _, _, s, t = buffers[q]
        (d0, r0), (d1, r1) = (order[step] for order in parts[q][2])
        peer = ((1 - c) * flip(me_d, d0) + c * flip(me_d, d1), (1 - c) * flip(me_r, r0) + c * flip(me_r, r1))
        return rcopy(acc.at[r], got.at[r], s.at[r], t.at[r], peer)

    bases = [4 * blocks * sum(p[1] for p in parts[:q]) for q in range(len(parts))]

    def local(q, other, r, put):
        words = 2 * parts[q][1]
        at = pl.ds(bases[q] + (other * blocks + r) * words, words)
        v = tabs[0][at, :]
        for tab in tabs[1:]:
            v = v + tab[at, :]
        put(slice(0, words), v)
        if q == 0:
            put(slice(words, words + 1), cnt_ref[pl.ds(other * blocks + r, 1), :])

    def total(q, r, step, put):
        _, come, _, got = buffers[q][:4]
        across(q, r).wait_recv()
        come_from = [come.at[r]]
        for k in range(step):
            at = r + (blocks >> (k + 1))
            message(q, at, k).wait_recv()
            come_from.append(got.at[at])

        def add(rows, v):
            for ref in come_from:
                v = v + ref[rows, :]
            put(rows, v)

        local(q, 0, r, add)

    def into(ref, r):
        def put(rows, v):
            ref[r, rows, :] = v
        return put

    pl.semaphore_wait(barrier, len(peers))

    def forward(q, r):
        step = depth - r.bit_length()
        total(q, r, step, into(buffers[q][2], r))
        message(q, r, step).start()

    order = turns(blocks, parts)
    lead = next(n for n, (q, r) in enumerate(order) if r < blocks // 2)
    for n, (q, r) in enumerate(order):
        local(q, 1, r, into(buffers[q][0], r))
        across(q, r).start()
        if LAG <= n < lead + LAG:
            forward(*order[n - LAG])
    for q, r in order[lead:]:
        if r:
            forward(q, r)

    for q in reversed(range(len(parts))):
        first, keys, _ = parts[q]

        def put(rows, v):
            if rows.start < 2 * keys:
                final[2 * first:2 * (first + keys), :] = v
            else:
                final[2 * kpd:2 * kpd + 1, :] = v

        total(q, 0, depth, put)
    cf = final[2 * kpd:2 * kpd + 1, 0:kpd]
    cout_ref[...] = cf
    spread = jnp.broadcast_to(jnp.maximum(cf, 1.0), (kpd, kpd))
    eye = lax.broadcasted_iota(jnp.int32, (kpd, kpd), 0) == lax.broadcasted_iota(jnp.int32, (kpd, kpd), 1)
    col = jnp.sum(jnp.where(eye, spread, 0.0), axis=1, keepdims=True)
    out_ref[:, 0:LANES] = final[pl.ds(0, kpd, stride=2), :] / col
    out_ref[:, LANES:2 * LANES] = final[pl.ds(1, kpd, stride=2), :] / col

    @pl.loop(0, blocks)
    def _(r):
        for q in range(len(parts)):
            across(q, r).wait_send()

    for step in range(depth):
        size = blocks >> (step + 1)

        @pl.loop(size, 2 * size)
        def _(r):
            for q in range(len(parts)):
                message(q, r, step).wait_send()


def per_device(facts, row_owner, key_offset):
    n_dom, n_rep = lax.axis_size("dom"), lax.axis_size("rep")
    rows, M = facts.shape
    blocks = n_dom * n_rep // 2
    kpd = KEYS // (n_dom * n_rep)
    parts = routes(n_dom, n_rep, kpd)
    nchunks = 2

    def vm(*shape, dtype=F32):
        return pltpu.VMEM(shape, dtype)

    def dma(*shape):
        return [pltpu.SemaphoreType.DMA(shape)] * 2 if shape else [pltpu.SemaphoreType.DMA] * 2

    I32 = jnp.int32
    pin = pltpu.with_memory_space_constraint
    hbm = pl.BlockSpec(memory_space=pltpu.HBM)
    vmem = pl.BlockSpec(memory_space=pltpu.VMEM)
    by_tile = facts.reshape(rows // 8, 8, 2, LANES).transpose(0, 2, 1, 3).reshape(2 * rows, LANES)
    square = (rows // LANES, LANES)
    ints = [row_owner.reshape(square), key_offset.reshape(square), row_owner.reshape(1, rows), key_offset.reshape(1, rows)]
    *tables, counted = pl.pallas_call(
        functools.partial(scatter, parts, n_dom, n_rep, rows),
        out_shape=[vm(2 * KEYS, LANES)] * TABLES + [vm(2 * blocks, LANES)],
        in_specs=[hbm] * 5,
        out_specs=[vmem] * (TABLES + 1),
        scratch_shapes=[
            vm(*square, dtype=I32), vm(*square, dtype=I32), vm(1, rows, dtype=I32), vm(1, rows, dtype=I32),
            vm(*square, dtype=I32), pltpu.SMEM(square, I32), vm(2 * rows, LANES),
            pltpu.SemaphoreType.DMA((4,)), pltpu.SemaphoreType.DMA, pltpu.SemaphoreType.DMA((nchunks,)),
        ],
        compiler_params=pltpu.CompilerParams(vmem_limit_bytes=8 * 1024 * 1024),
    )(*(pin(a, pltpu.HBM) for a in ints + [by_tile]))

    scratch = [vm(2 * kpd + 8, LANES)]
    for q, (_, keys, _) in enumerate(parts):
        scratch += [vm(blocks, 2 * keys + (q == 0), LANES)] * 4 + dma(blocks) + dma(blocks)
    means, counts = pl.pallas_call(
        functools.partial(kernel, parts, n_dom, n_rep),
        out_shape=(vm(kpd, M), vm(1, kpd)),
        in_specs=[vmem] * (TABLES + 1),
        out_specs=(vmem, vmem),
        scratch_shapes=scratch,
        compiler_params=pltpu.CompilerParams(
            collective_id=0, has_side_effects=True, vmem_limit_bytes=16 * 1024 * 1024
        ),
    )(*(pin(a, pltpu.VMEM) for a in (counted, *tables)))
    return means, counts.reshape(kpd)


def solution(mesh):
    placed = (P(("dom", "rep"), None), P(("dom", "rep"), None), P(("dom", "rep")))
    return jax.shard_map(
        per_device,
        mesh=mesh,
        in_specs=placed,
        out_specs=(P(("dom", "rep"), None), P(("dom", "rep"))),
        check_vma=False,
    )
```

```python
import functools

import jax
import jax.numpy as jnp
from jax import lax
from jax.experimental import pallas as pl
from jax.experimental.pallas import tpu as pltpu
from jax.sharding import PartitionSpec as P

KEYS = 4096
MESH = pl.DeviceIdType.MESH
F32 = jnp.float32
BF16 = jnp.bfloat16
LANES = 128
TABLES = 7
LAG = 8
TURNS = (
    31, 40, 15, 29, 30, 47, 45, 44, 27, 46, 23, 7, 41, 11, 39, 25,
    13, 37, 14, 43, 19, 26, 21, 3, 22, 36, 9, 38, 5, 6, 28, 17,
    42, 10, 12, 18, 24, 35, 8, 1, 20, 2, 34, 33, 4, 32, 16, 0,
)


def flip(index, bits):
    at = 1
    while at <= bits:
        if bits & at:
            index = index + at * (1 - 2 * ((index // at) % 2))
        at *= 2
    return index


def log2(n):
    return n.bit_length() - 1


def routes(n_dom, n_rep, kpd):
    x, y = (0, 1), (2, 0)
    rest = [(1 << b, 0) for b in range(2, log2(n_dom))] + [(0, 1 << b) for b in range(1, log2(n_rep))]
    flat, tall = ([x, y, *rest], [y, x, *rest]), ([*rest, y, x], [*rest, x, y])
    cuts = [kpd * at // 128 // 4 * 4 for at in (0, 52, 100)] + [kpd]
    ways = [flat, flat, tall]
    return [(cuts[q], cuts[q + 1] - cuts[q], way) for q, way in enumerate(ways) if cuts[q] < cuts[q + 1]]


def turns(blocks, parts):
    if blocks == 16 and len(parts) == 3:
        return [divmod(turn, 16) for turn in TURNS]
    return [(q, r) for r in reversed(range(blocks)) for q in range(len(parts))]


def label(orders, n_dom, n_rep, me_d, me_r, owner, rep):
    rel_d, rel_r = owner ^ me_d, rep ^ me_r
    found = []
    for order in orders:
        r = rel_d & 1
        for bit_d, bit_r in order:
            bit = rel_d >> log2(bit_d) if bit_d else rel_r >> log2(bit_r)
            r = 2 * r + (bit & 1)
        found.append(r)
    return jnp.where((owner & 1) == 0, found[0], found[1])


def scatter(parts, n_dom, n_rep, rows, owner_hbm, offset_hbm, owner_row_hbm, offset_row_hbm, facts_hbm, *refs):
    tabs, refs = refs[:TABLES], refs[TABLES:]
    cnt_ref, owner_ref, offset_ref, owner_row, offset_row, lab_ref, at_ref, fbuf, isem, lsem, fsem = refs
    me_d, me_r = lax.axis_index("dom"), lax.axis_index("rep")
    blocks = n_dom * n_rep // 2
    kpd = KEYS // (2 * blocks)
    nchunks = fsem.shape[0]
    words = 2 * rows // nchunks
    ints = [
        pltpu.make_async_copy(src, dst, isem.at[k])
        for k, (src, dst) in enumerate(
            [(owner_hbm, owner_ref), (offset_hbm, offset_ref), (owner_row_hbm, owner_row), (offset_row_hbm, offset_row)]
        )
    ]
    loads = [
        pltpu.make_async_copy(
            facts_hbm.at[pl.ds(k * words, words)], fbuf.at[pl.ds(k * words, words)], fsem.at[k]
        )
        for k in range(nchunks)
    ]
    for ld in ints + loads:
        ld.start()

    def clear(first, last):
        @pl.loop(0, KEYS // 64)
        def _(i):
            at = pl.ds(pl.multiple_of(i * 128, 128), 128)
            for tab in tabs[first:last]:
                tab[at, :] = jnp.zeros((128, LANES), F32)

    clear(0, TABLES // 2)
    for ld in ints[:2]:
        ld.wait()
    owner, offset = owner_ref[...], offset_ref[...]
    i, base, word = offset & (kpd - 1), 0, None
    for first, keys, orders in parts:
        r = label(orders, n_dom, n_rep, me_d, me_r, owner, offset >> log2(kpd))
        at = base + 2 * (r * keys + i - first)
        word = at if word is None else jnp.where(i >= first, at, word)
        base += 4 * blocks * keys
    lab_ref[...] = word
    labels = pltpu.make_async_copy(lab_ref, at_ref, lsem)
    labels.start()
    clear(TABLES // 2, TABLES)
    for ld in ints[2:]:
        ld.wait()
    owner, offset = owner_row[...], offset_row[...]
    r = label(parts[0][2], n_dom, n_rep, me_d, me_r, owner, offset >> log2(kpd))
    i = offset & (kpd - 1)
    hot_r = jnp.where(lax.broadcasted_iota(jnp.int32, (2 * blocks, rows), 0) == r, 1.0, 0.0).astype(BF16)
    hot_i = jnp.where(lax.broadcasted_iota(jnp.int32, (LANES, rows), 0) == i, 1.0, 0.0).astype(BF16)
    cnt_ref[...] = lax.dot_general(hot_r, hot_i, (((1,), (1,)), ((), ())), preferred_element_type=F32)

    labels.wait()
    group = rows // nchunks // LANES
    for k in range(nchunks):
        loads[k].wait()

        @pl.loop(0, group)
        def _(g):
            base = pl.multiple_of((k * group + g) * 2 * LANES, 2 * LANES)
            mine = at_ref.at[k * group + g]
            for r in range(LANES):
                at = pl.ds(pl.multiple_of(mine[r], 2), 2)
                row = fbuf[pl.ds(base + 16 * (r // 8) + r % 8, 2, stride=8), :]
                tabs[r % TABLES][at, :] = tabs[r % TABLES][at, :] + row


def kernel(parts, n_dom, n_rep, cnt_ref, *refs):
    blocks = n_dom * n_rep // 2
    kpd = KEYS // (n_dom * n_rep)
    depth = log2(blocks)
    tabs, (final, *refs) = refs[:TABLES], refs[TABLES:]
    buffers = [refs[8 * q:8 * q + 8] for q in range(len(parts))]
    me_d, me_r = lax.axis_index("dom"), lax.axis_index("rep")
    c = me_d % 2
    core = (flip(me_d, 1), me_r)
    peers = [core] + [(flip(me_d, d), flip(me_r, r)) for d, r in parts[0][2][0]]
    barrier = pltpu.get_barrier_semaphore()
    for p in peers:
        pl.semaphore_signal(barrier, inc=1, device_id=p, device_id_type=MESH)

    def rcopy(src, dst, s, t, dev):
        return pltpu.make_async_remote_copy(
            src_ref=src, dst_ref=dst, send_sem=s, recv_sem=t, device_id=dev, device_id_type=MESH
        )

    def across(q, r):
        out, come, _, _, s, t, _, _ = buffers[q]
        return rcopy(out.at[r], come.at[r], s.at[r], t.at[r], core)

    def message(q, r, step):
        _, _, acc, got, _, _, s, t = buffers[q]
        (d0, r0), (d1, r1) = (order[step] for order in parts[q][2])
        peer = ((1 - c) * flip(me_d, d0) + c * flip(me_d, d1), (1 - c) * flip(me_r, r0) + c * flip(me_r, r1))
        return rcopy(acc.at[r], got.at[r], s.at[r], t.at[r], peer)

    bases = [4 * blocks * sum(p[1] for p in parts[:q]) for q in range(len(parts))]

    def local(q, other, r, put):
        words = 2 * parts[q][1]
        at = pl.ds(bases[q] + (other * blocks + r) * words, words)
        v = tabs[0][at, :]
        for tab in tabs[1:]:
            v = v + tab[at, :]
        put(slice(0, words), v)
        if q == 0:
            put(slice(words, words + 1), cnt_ref[pl.ds(other * blocks + r, 1), :])

    def total(q, r, step, put):
        _, come, _, got = buffers[q][:4]
        across(q, r).wait_recv()
        come_from = [come.at[r]]
        for k in range(step):
            at = r + (blocks >> (k + 1))
            message(q, at, k).wait_recv()
            come_from.append(got.at[at])

        def add(rows, v):
            for ref in come_from:
                v = v + ref[rows, :]
            put(rows, v)

        local(q, 0, r, add)

    def into(ref, r):
        def put(rows, v):
            ref[r, rows, :] = v
        return put

    pl.semaphore_wait(barrier, len(peers))

    def forward(q, r):
        step = depth - r.bit_length()
        total(q, r, step, into(buffers[q][2], r))
        message(q, r, step).start()

    order = turns(blocks, parts)
    lead = next(n for n, (q, r) in enumerate(order) if r < blocks // 2)
    for n, (q, r) in enumerate(order):
        local(q, 1, r, into(buffers[q][0], r))
        across(q, r).start()
        if LAG <= n < lead + LAG:
            forward(*order[n - LAG])
    for q, r in order[lead:]:
        if r:
            forward(q, r)

    @pl.loop(0, blocks)
    def _(r):
        for q in range(len(parts)):
            across(q, r).wait_send()

    for step in range(depth):
        size = blocks >> (step + 1)

        @pl.loop(size, 2 * size)
        def _(r):
            for q in range(len(parts)):
                message(q, r, step).wait_send()

    for q in reversed(range(len(parts))):
        first, keys, _ = parts[q]

        def put(rows, v):
            if rows.start < 2 * keys:
                final[2 * first:2 * (first + keys), :] = v
            else:
                final[2 * kpd:2 * kpd + 1, :] = v

        total(q, 0, depth, put)


def divide(kpd, final, out_hbm, cout_hbm, out_ref, cout_ref, osem):
    cf = final[2 * kpd:2 * kpd + 1, 0:kpd]
    cout_ref[...] = cf
    copies = [pltpu.make_async_copy(cout_ref, cout_hbm, osem.at[0]), pltpu.make_async_copy(out_ref, out_hbm, osem.at[1])]
    copies[0].start()
    spread = jnp.broadcast_to(jnp.maximum(cf, 1.0), (kpd, kpd))
    eye = lax.broadcasted_iota(jnp.int32, (kpd, kpd), 0) == lax.broadcasted_iota(jnp.int32, (kpd, kpd), 1)
    col = jnp.sum(jnp.where(eye, spread, 0.0), axis=1, keepdims=True)
    out_ref[:, 0:LANES] = final[pl.ds(0, kpd, stride=2), :] / col
    out_ref[:, LANES:2 * LANES] = final[pl.ds(1, kpd, stride=2), :] / col
    copies[1].start()
    for cp in copies:
        cp.wait()


def per_device(facts, row_owner, key_offset):
    n_dom, n_rep = lax.axis_size("dom"), lax.axis_size("rep")
    rows, M = facts.shape
    blocks = n_dom * n_rep // 2
    kpd = KEYS // (n_dom * n_rep)
    parts = routes(n_dom, n_rep, kpd)
    nchunks = 2

    def vm(*shape, dtype=F32):
        return pltpu.VMEM(shape, dtype)

    def dma(*shape):
        return [pltpu.SemaphoreType.DMA(shape)] * 2 if shape else [pltpu.SemaphoreType.DMA] * 2

    I32 = jnp.int32
    pin = pltpu.with_memory_space_constraint
    hbm = pl.BlockSpec(memory_space=pltpu.HBM)
    vmem = pl.BlockSpec(memory_space=pltpu.VMEM)
    by_tile = facts.reshape(rows // 8, 8, 2, LANES).transpose(0, 2, 1, 3).reshape(2 * rows, LANES)
    square = (rows // LANES, LANES)
    ints = [row_owner.reshape(square), key_offset.reshape(square), row_owner.reshape(1, rows), key_offset.reshape(1, rows)]
    *tables, counted = pl.pallas_call(
        functools.partial(scatter, parts, n_dom, n_rep, rows),
        out_shape=[vm(2 * KEYS, LANES)] * TABLES + [vm(2 * blocks, LANES)],
        in_specs=[hbm] * 5,
        out_specs=[vmem] * (TABLES + 1),
        scratch_shapes=[
            vm(*square, dtype=I32), vm(*square, dtype=I32), vm(1, rows, dtype=I32), vm(1, rows, dtype=I32),
            vm(*square, dtype=I32), pltpu.SMEM(square, I32), vm(2 * rows, LANES),
            pltpu.SemaphoreType.DMA((4,)), pltpu.SemaphoreType.DMA, pltpu.SemaphoreType.DMA((nchunks,)),
        ],
        compiler_params=pltpu.CompilerParams(vmem_limit_bytes=8 * 1024 * 1024),
    )(*(pin(a, pltpu.HBM) for a in ints + [by_tile]))

    scratch = []
    for q, (_, keys, _) in enumerate(parts):
        scratch += [vm(blocks, 2 * keys + (q == 0), LANES)] * 4 + dma(blocks) + dma(blocks)
    final = pl.pallas_call(
        functools.partial(kernel, parts, n_dom, n_rep),
        out_shape=vm(2 * kpd + 8, LANES),
        in_specs=[vmem] * (TABLES + 1),
        out_specs=vmem,
        scratch_shapes=scratch,
        compiler_params=pltpu.CompilerParams(
            collective_id=0, has_side_effects=True, vmem_limit_bytes=16 * 1024 * 1024
        ),
    )(*(pin(a, pltpu.VMEM) for a in (counted, *tables)))
    means, counts = pl.pallas_call(
        functools.partial(divide, kpd),
        out_shape=(jax.ShapeDtypeStruct((kpd, M), F32), jax.ShapeDtypeStruct((1, kpd), F32)),
        in_specs=[vmem],
        out_specs=(hbm, hbm),
        scratch_shapes=[vm(kpd, M), vm(1, kpd), pltpu.SemaphoreType.DMA((2,))],
        compiler_params=pltpu.CompilerParams(vmem_limit_bytes=4 * 1024 * 1024),
    )(pin(final, pltpu.VMEM))
    return means, counts.reshape(kpd)


def solution(mesh):
    placed = (P(("dom", "rep"), None), P(("dom", "rep"), None), P(("dom", "rep")))
    return jax.shard_map(
        per_device,
        mesh=mesh,
        in_specs=placed,
        out_specs=(P(("dom", "rep"), None), P(("dom", "rep"))),
        check_vma=False,
    )
```

```python
import functools

import jax
import jax.numpy as jnp
from jax import lax
from jax.experimental import pallas as pl
from jax.experimental.pallas import tpu as pltpu
from jax.sharding import PartitionSpec as P

KEYS = 4096
MESH = pl.DeviceIdType.MESH
F32 = jnp.float32
BF16 = jnp.bfloat16
LANES = 128
TABLES = 7
LAG = 8
TURNS = (
    31, 40, 15, 29, 30, 47, 45, 44, 27, 46, 23, 7, 41, 11, 39, 25,
    13, 37, 14, 43, 19, 26, 21, 3, 22, 36, 9, 38, 5, 6, 28, 17,
    42, 10, 12, 18, 24, 35, 8, 1, 20, 2, 34, 33, 4, 32, 16, 0,
)


def flip(index, bits):
    at = 1
    while at <= bits:
        if bits & at:
            index = index + at * (1 - 2 * ((index // at) % 2))
        at *= 2
    return index


def log2(n):
    return n.bit_length() - 1


def routes(n_dom, n_rep, kpd):
    x, y = (0, 1), (2, 0)
    rest = [(1 << b, 0) for b in range(2, log2(n_dom))] + [(0, 1 << b) for b in range(1, log2(n_rep))]
    flat, tall = ([x, y, *rest], [y, x, *rest]), ([*rest, y, x], [*rest, x, y])
    cuts = [kpd * at // 128 // 4 * 4 for at in (0, 52, 100)] + [kpd]
    ways = [flat, flat, tall]
    return [(cuts[q], cuts[q + 1] - cuts[q], way) for q, way in enumerate(ways) if cuts[q] < cuts[q + 1]]


def turns(blocks, parts):
    if blocks == 16 and len(parts) == 3:
        return [divmod(turn, 16) for turn in TURNS]
    return [(q, r) for r in reversed(range(blocks)) for q in range(len(parts))]


def label(orders, n_dom, n_rep, me_d, me_r, owner, rep):
    rel_d, rel_r = owner ^ me_d, rep ^ me_r
    found = []
    for order in orders:
        r = rel_d & 1
        for bit_d, bit_r in order:
            bit = rel_d >> log2(bit_d) if bit_d else rel_r >> log2(bit_r)
            r = 2 * r + (bit & 1)
        found.append(r)
    return jnp.where((owner & 1) == 0, found[0], found[1])


def scatter(parts, n_dom, n_rep, rows, owner_hbm, offset_hbm, owner_row_hbm, offset_row_hbm, facts_hbm, *refs):
    tabs, refs = refs[:TABLES], refs[TABLES:]
    cnt_ref, owner_ref, offset_ref, owner_row, offset_row, lab_ref, at_ref, fbuf, isem, lsem, fsem = refs
    me_d, me_r = lax.axis_index("dom"), lax.axis_index("rep")
    blocks = n_dom * n_rep // 2
    kpd = KEYS // (2 * blocks)
    nchunks = fsem.shape[0]
    words = 2 * rows // nchunks
    ints = [
        pltpu.make_async_copy(src, dst, isem.at[k])
        for k, (src, dst) in enumerate(
            [(owner_hbm, owner_ref), (offset_hbm, offset_ref), (owner_row_hbm, owner_row), (offset_row_hbm, offset_row)]
        )
    ]
    loads = [
        pltpu.make_async_copy(
            facts_hbm.at[pl.ds(k * words, words)], fbuf.at[pl.ds(k * words, words)], fsem.at[k]
        )
        for k in range(nchunks)
    ]
    for ld in ints + loads:
        ld.start()

    def clear(first, last):
        @pl.loop(0, KEYS // 64)
        def _(i):
            at = pl.ds(pl.multiple_of(i * 128, 128), 128)
            for tab in tabs[first:last]:
                tab[at, :] = jnp.zeros((128, LANES), F32)

    clear(0, TABLES // 2)
    for ld in ints[:2]:
        ld.wait()
    owner, offset = owner_ref[...], offset_ref[...]
    i, base, word = offset & (kpd - 1), 0, None
    for first, keys, orders in parts:
        r = label(orders, n_dom, n_rep, me_d, me_r, owner, offset >> log2(kpd))
        at = base + 2 * (r * keys + i - first)
        word = at if word is None else jnp.where(i >= first, at, word)
        base += 4 * blocks * keys
    lab_ref[...] = word
    labels = pltpu.make_async_copy(lab_ref, at_ref, lsem)
    labels.start()
    clear(TABLES // 2, TABLES)
    for ld in ints[2:]:
        ld.wait()
    owner, offset = owner_row[...], offset_row[...]
    r = label(parts[0][2], n_dom, n_rep, me_d, me_r, owner, offset >> log2(kpd))
    i = offset & (kpd - 1)
    hot_r = jnp.where(lax.broadcasted_iota(jnp.int32, (2 * blocks, rows), 0) == r, 1.0, 0.0).astype(BF16)
    hot_i = jnp.where(lax.broadcasted_iota(jnp.int32, (LANES, rows), 0) == i, 1.0, 0.0).astype(BF16)
    cnt_ref[...] = lax.dot_general(hot_r, hot_i, (((1,), (1,)), ((), ())), preferred_element_type=F32)

    labels.wait()
    group = rows // nchunks // LANES
    for k in range(nchunks):
        loads[k].wait()

        @pl.loop(0, group)
        def _(g):
            base = pl.multiple_of((k * group + g) * 2 * LANES, 2 * LANES)
            mine = at_ref.at[k * group + g]
            for r in range(LANES):
                at = pl.ds(pl.multiple_of(mine[r], 2), 2)
                row = fbuf[pl.ds(base + 16 * (r // 8) + r % 8, 2, stride=8), :]
                tabs[r % TABLES][at, :] = tabs[r % TABLES][at, :] + row


def kernel(parts, n_dom, n_rep, cnt_ref, *refs):
    blocks = n_dom * n_rep // 2
    kpd = KEYS // (n_dom * n_rep)
    depth = log2(blocks)
    tabs, (final, *refs) = refs[:TABLES], refs[TABLES:]
    buffers = [refs[8 * q:8 * q + 8] for q in range(len(parts))]
    me_d, me_r = lax.axis_index("dom"), lax.axis_index("rep")
    c = me_d % 2
    core = (flip(me_d, 1), me_r)
    peers = [core] + [(flip(me_d, d), flip(me_r, r)) for d, r in parts[0][2][0]]
    barrier = pltpu.get_barrier_semaphore()
    for p in peers:
        pl.semaphore_signal(barrier, inc=1, device_id=p, device_id_type=MESH)

    def rcopy(src, dst, s, t, dev):
        return pltpu.make_async_remote_copy(
            src_ref=src, dst_ref=dst, send_sem=s, recv_sem=t, device_id=dev, device_id_type=MESH
        )

    half = blocks // 2

    def across(q, r):
        out, come, _, _, s, t, _, _ = buffers[q]
        return rcopy(out.at[r], come.at[r], s, t.at[r], core)

    def message(q, r):
        _, _, acc, got, _, _, s, t = buffers[q]
        step = depth - r.bit_length()
        (d0, r0), (d1, r1) = (order[step] for order in parts[q][2])
        peer = ((1 - c) * flip(me_d, d0) + c * flip(me_d, d1), (1 - c) * flip(me_r, r0) + c * flip(me_r, r1))
        return rcopy(acc.at[r], got.at[r], s, t.at[r - (half >> step)], peer)

    def arrived(q, r, n):
        _, _, acc, got, _, _, s, t = buffers[q]
        rcopy(acc.at[pl.ds(0, n)], got.at[pl.ds(0, n)], s, t.at[r], core).wait_recv()

    bases = [4 * blocks * sum(p[1] for p in parts[:q]) for q in range(len(parts))]

    def local(q, other, r, put):
        words = 2 * parts[q][1]
        at = pl.ds(bases[q] + (other * blocks + r) * words, words)
        v = tabs[0][at, :]
        for tab in tabs[1:]:
            v = v + tab[at, :]
        put(slice(0, words), v)
        if q == 0:
            put(slice(words, words + 1), cnt_ref[pl.ds(other * blocks + r, 1), :])

    def total(q, r, put):
        _, come, _, got = buffers[q][:4]
        across(q, r).wait_recv()
        come_from = [come.at[r]]
        step = depth - r.bit_length()
        if step:
            arrived(q, r, step)
        for k in range(step):
            come_from.append(got.at[r + (half >> k)])

        def add(rows, v):
            for ref in come_from:
                v = v + ref[rows, :]
            put(rows, v)

        local(q, 0, r, add)

    def into(ref, r):
        def put(rows, v):
            ref[r, rows, :] = v
        return put

    pl.semaphore_wait(barrier, len(peers))

    def forward(q, r):
        total(q, r, into(buffers[q][2], r))
        message(q, r).start()

    order = turns(blocks, parts)
    lead = next(n for n, (q, r) in enumerate(order) if r < half)
    for n, (q, r) in enumerate(order):
        local(q, 1, r, into(buffers[q][0], r))
        across(q, r).start()
        if LAG <= n < lead + LAG:
            forward(*order[n - LAG])
    for q, r in order[min(lead, len(order) - LAG):]:
        if r:
            forward(q, r)
    for q in range(len(parts)):
        out, come, acc, got, s, t, s2, t2 = buffers[q]
        rcopy(out, come, s, t.at[0], core).wait_send()
        rest = pl.ds(1, blocks - 1)
        rcopy(acc.at[rest], got.at[rest], s2, t2.at[0], core).wait_send()

    for q in reversed(range(len(parts))):
        first, keys, _ = parts[q]

        def put(rows, v):
            if rows.start < 2 * keys:
                final[2 * first:2 * (first + keys), :] = v
            else:
                final[2 * kpd:2 * kpd + 1, :] = v

        total(q, 0, put)


def divide(kpd, final, out_hbm, cout_hbm, out_ref, cout_ref, osem):
    cf = final[2 * kpd:2 * kpd + 1, 0:kpd]
    cout_ref[...] = cf
    copies = [pltpu.make_async_copy(cout_ref, cout_hbm, osem.at[0]), pltpu.make_async_copy(out_ref, out_hbm, osem.at[1])]
    copies[0].start()
    spread = jnp.broadcast_to(jnp.maximum(cf, 1.0), (kpd, kpd))
    eye = lax.broadcasted_iota(jnp.int32, (kpd, kpd), 0) == lax.broadcasted_iota(jnp.int32, (kpd, kpd), 1)
    col = jnp.sum(jnp.where(eye, spread, 0.0), axis=1, keepdims=True)
    out_ref[:, 0:LANES] = final[pl.ds(0, kpd, stride=2), :] / col
    out_ref[:, LANES:2 * LANES] = final[pl.ds(1, kpd, stride=2), :] / col
    copies[1].start()
    for cp in copies:
        cp.wait()


def per_device(facts, row_owner, key_offset):
    n_dom, n_rep = lax.axis_size("dom"), lax.axis_size("rep")
    rows, M = facts.shape
    blocks = n_dom * n_rep // 2
    kpd = KEYS // (n_dom * n_rep)
    parts = routes(n_dom, n_rep, kpd)
    nchunks = 2

    def vm(*shape, dtype=F32):
        return pltpu.VMEM(shape, dtype)

    def dma(*shape):
        return pltpu.SemaphoreType.DMA(shape) if shape else pltpu.SemaphoreType.DMA

    I32 = jnp.int32
    pin = pltpu.with_memory_space_constraint
    hbm = pl.BlockSpec(memory_space=pltpu.HBM)
    vmem = pl.BlockSpec(memory_space=pltpu.VMEM)
    by_tile = facts.reshape(rows // 8, 8, 2, LANES).transpose(0, 2, 1, 3).reshape(2 * rows, LANES)
    square = (rows // LANES, LANES)
    ints = [row_owner.reshape(square), key_offset.reshape(square), row_owner.reshape(1, rows), key_offset.reshape(1, rows)]
    *tables, counted = pl.pallas_call(
        functools.partial(scatter, parts, n_dom, n_rep, rows),
        out_shape=[vm(2 * KEYS, LANES)] * TABLES + [vm(2 * blocks, LANES)],
        in_specs=[hbm] * 5,
        out_specs=[vmem] * (TABLES + 1),
        scratch_shapes=[
            vm(*square, dtype=I32), vm(*square, dtype=I32), vm(1, rows, dtype=I32), vm(1, rows, dtype=I32),
            vm(*square, dtype=I32), pltpu.SMEM(square, I32), vm(2 * rows, LANES),
            pltpu.SemaphoreType.DMA((4,)), pltpu.SemaphoreType.DMA, pltpu.SemaphoreType.DMA((nchunks,)),
        ],
        compiler_params=pltpu.CompilerParams(vmem_limit_bytes=8 * 1024 * 1024),
    )(*(pin(a, pltpu.HBM) for a in ints + [by_tile]))

    scratch = []
    for q, (_, keys, _) in enumerate(parts):
        scratch += [vm(blocks, 2 * keys + (q == 0), LANES)] * 4
        scratch += [dma(), dma(blocks), dma(), dma(blocks // 2)]
    final = pl.pallas_call(
        functools.partial(kernel, parts, n_dom, n_rep),
        out_shape=vm(2 * kpd + 8, LANES),
        in_specs=[vmem] * (TABLES + 1),
        out_specs=vmem,
        scratch_shapes=scratch,
        compiler_params=pltpu.CompilerParams(
            collective_id=0, has_side_effects=True, vmem_limit_bytes=16 * 1024 * 1024
        ),
    )(*(pin(a, pltpu.VMEM) for a in (counted, *tables)))
    means, counts = pl.pallas_call(
        functools.partial(divide, kpd),
        out_shape=(jax.ShapeDtypeStruct((kpd, M), F32), jax.ShapeDtypeStruct((1, kpd), F32)),
        in_specs=[vmem],
        out_specs=(hbm, hbm),
        scratch_shapes=[vm(kpd, M), vm(1, kpd), pltpu.SemaphoreType.DMA((2,))],
        compiler_params=pltpu.CompilerParams(vmem_limit_bytes=4 * 1024 * 1024),
    )(pin(final, pltpu.VMEM))
    return means, counts.reshape(kpd)


def solution(mesh):
    placed = (P(("dom", "rep"), None), P(("dom", "rep"), None), P(("dom", "rep")))
    return jax.shard_map(
        per_device,
        mesh=mesh,
        in_specs=placed,
        out_specs=(P(("dom", "rep"), None), P(("dom", "rep"))),
        check_vma=False,
    )
```

```python
import functools

import jax
import jax.numpy as jnp
from jax import lax
from jax.experimental import pallas as pl
from jax.experimental.pallas import tpu as pltpu
from jax.sharding import PartitionSpec as P

KEYS = 4096
MESH = pl.DeviceIdType.MESH
F32 = jnp.float32
BF16 = jnp.bfloat16
LANES = 128
TABLES = 7
LAG = 8
TURNS = (
    31, 44, 46, 15, 63, 14, 27, 40, 60, 47, 29, 45, 43, 62, 59, 23,
    36, 55, 13, 11, 57, 30, 25, 52, 58, 10, 7, 39, 61, 9, 21, 6,
    12, 37, 26, 19, 56, 28, 5, 54, 53, 51, 8, 3, 22, 38, 42, 41,
    17, 35, 2, 50, 1, 24, 4, 33, 49, 18, 34, 20, 48, 32, 16, 0,
)


def flip(index, bits):
    at = 1
    while at <= bits:
        if bits & at:
            index = index + at * (1 - 2 * ((index // at) % 2))
        at *= 2
    return index


def log2(n):
    return n.bit_length() - 1


def routes(n_dom, n_rep, kpd):
    x, y = (0, 1), (2, 0)
    rest = [(1 << b, 0) for b in range(2, log2(n_dom))] + [(0, 1 << b) for b in range(1, log2(n_rep))]
    flat, tall = ([x, y, *rest], [y, x, *rest]), ([*rest, y, x], [*rest, x, y])
    cuts = [kpd * at // 128 // 4 * 4 for at in (0, 52, 100, 116)] + [kpd]
    ways = [flat, flat, tall, tall]
    return [(cuts[q], cuts[q + 1] - cuts[q], way) for q, way in enumerate(ways) if cuts[q] < cuts[q + 1]]


def turns(blocks, parts):
    if blocks == 16 and len(parts) == 4:
        return [divmod(turn, 16) for turn in TURNS]
    return [(q, r) for r in reversed(range(blocks)) for q in range(len(parts))]


def label(orders, n_dom, n_rep, me_d, me_r, owner, rep):
    rel_d, rel_r = owner ^ me_d, rep ^ me_r
    found = []
    for order in orders:
        r = rel_d & 1
        for bit_d, bit_r in order:
            bit = rel_d >> log2(bit_d) if bit_d else rel_r >> log2(bit_r)
            r = 2 * r + (bit & 1)
        found.append(r)
    return jnp.where((owner & 1) == 0, found[0], found[1])


def scatter(parts, n_dom, n_rep, rows, owner_hbm, offset_hbm, owner_row_hbm, offset_row_hbm, facts_hbm, *refs):
    tabs, refs = refs[:TABLES], refs[TABLES:]
    cnt_ref, owner_ref, offset_ref, owner_row, offset_row, lab_ref, at_ref, fbuf, isem, lsem, fsem = refs
    me_d, me_r = lax.axis_index("dom"), lax.axis_index("rep")
    blocks = n_dom * n_rep // 2
    kpd = KEYS // (2 * blocks)
    nchunks = fsem.shape[0]
    words = 2 * rows // nchunks
    ints = [
        pltpu.make_async_copy(src, dst, isem.at[k])
        for k, (src, dst) in enumerate(
            [(owner_hbm, owner_ref), (offset_hbm, offset_ref), (owner_row_hbm, owner_row), (offset_row_hbm, offset_row)]
        )
    ]
    loads = [
        pltpu.make_async_copy(
            facts_hbm.at[pl.ds(k * words, words)], fbuf.at[pl.ds(k * words, words)], fsem.at[k]
        )
        for k in range(nchunks)
    ]
    for ld in ints + loads:
        ld.start()

    def clear(first, last):
        @pl.loop(0, KEYS // 64)
        def _(i):
            at = pl.ds(pl.multiple_of(i * 128, 128), 128)
            for tab in tabs[first:last]:
                tab[at, :] = jnp.zeros((128, LANES), F32)

    clear(0, TABLES // 2)
    for ld in ints[:2]:
        ld.wait()
    owner, offset = owner_ref[...], offset_ref[...]
    i, base, word = offset & (kpd - 1), 0, None
    for first, keys, orders in parts:
        r = label(orders, n_dom, n_rep, me_d, me_r, owner, offset >> log2(kpd))
        at = base + 2 * (r * keys + i - first)
        word = at if word is None else jnp.where(i >= first, at, word)
        base += 4 * blocks * keys
    lab_ref[...] = word
    labels = pltpu.make_async_copy(lab_ref, at_ref, lsem)
    labels.start()
    clear(TABLES // 2, TABLES)
    for ld in ints[2:]:
        ld.wait()
    owner, offset = owner_row[...], offset_row[...]
    r = label(parts[0][2], n_dom, n_rep, me_d, me_r, owner, offset >> log2(kpd))
    i = offset & (kpd - 1)
    hot_r = jnp.where(lax.broadcasted_iota(jnp.int32, (2 * blocks, rows), 0) == r, 1.0, 0.0).astype(BF16)
    hot_i = jnp.where(lax.broadcasted_iota(jnp.int32, (LANES, rows), 0) == i, 1.0, 0.0).astype(BF16)
    cnt_ref[...] = lax.dot_general(hot_r, hot_i, (((1,), (1,)), ((), ())), preferred_element_type=F32)

    labels.wait()
    group = rows // nchunks // LANES
    for k in range(nchunks):
        loads[k].wait()

        @pl.loop(0, group)
        def _(g):
            base = pl.multiple_of((k * group + g) * 2 * LANES, 2 * LANES)
            mine = at_ref.at[k * group + g]
            for r in range(LANES):
                at = pl.ds(pl.multiple_of(mine[r], 2), 2)
                row = fbuf[pl.ds(base + 16 * (r // 8) + r % 8, 2, stride=8), :]
                tabs[r % TABLES][at, :] = tabs[r % TABLES][at, :] + row


def kernel(parts, n_dom, n_rep, cnt_ref, *refs):
    blocks = n_dom * n_rep // 2
    kpd = KEYS // (n_dom * n_rep)
    depth = log2(blocks)
    tabs, (final, *refs) = refs[:TABLES], refs[TABLES:]
    buffers = [refs[8 * q:8 * q + 8] for q in range(len(parts))]
    me_d, me_r = lax.axis_index("dom"), lax.axis_index("rep")
    c = me_d % 2
    core = (flip(me_d, 1), me_r)
    peers = [core] + [(flip(me_d, d), flip(me_r, r)) for d, r in parts[0][2][0]]
    barrier = pltpu.get_barrier_semaphore()
    for p in peers:
        pl.semaphore_signal(barrier, inc=1, device_id=p, device_id_type=MESH)

    def rcopy(src, dst, s, t, dev):
        return pltpu.make_async_remote_copy(
            src_ref=src, dst_ref=dst, send_sem=s, recv_sem=t, device_id=dev, device_id_type=MESH
        )

    half = blocks // 2

    def across(q, r):
        out, come, _, _, s, t, _, _ = buffers[q]
        at, n = (r, r - half // 2) if r >= half else (pl.ds(r // 2 * 2, 2), r // 2)
        return rcopy(out.at[at], come.at[at], s, t.at[n], core)

    def message(q, r):
        _, _, acc, got, _, _, s, t = buffers[q]
        step = depth - r.bit_length()
        (d0, r0), (d1, r1) = (order[step] for order in parts[q][2])
        peer = ((1 - c) * flip(me_d, d0) + c * flip(me_d, d1), (1 - c) * flip(me_r, r0) + c * flip(me_r, r1))
        return rcopy(acc.at[r], got.at[r], s, t.at[r - (half >> step)], peer)

    def arrived(q, r, n):
        _, _, acc, got, _, _, s, t = buffers[q]
        rcopy(acc.at[pl.ds(0, n)], got.at[pl.ds(0, n)], s, t.at[r], core).wait_recv()

    bases = [4 * blocks * sum(p[1] for p in parts[:q]) for q in range(len(parts))]

    def local(q, other, r, put):
        words = 2 * parts[q][1]
        at = pl.ds(bases[q] + (other * blocks + r) * words, words)
        v = tabs[0][at, :]
        for tab in tabs[1:]:
            v = v + tab[at, :]
        put(slice(0, words), v)
        if q == 0:
            put(slice(words, words + 1), cnt_ref[pl.ds(other * blocks + r, 1), :])

    paired = set()

    def total(q, r, put):
        _, come, _, got = buffers[q][:4]
        if r >= half or (q, r // 2) not in paired:
            across(q, r).wait_recv()
            paired.add((q, r // 2))
        come_from = [come.at[r]]
        step = depth - r.bit_length()
        if step:
            arrived(q, r, step)
        for k in range(step):
            come_from.append(got.at[r + (half >> k)])

        def add(rows, v):
            for ref in come_from:
                v = v + ref[rows, :]
            put(rows, v)

        local(q, 0, r, add)

    def into(ref, r):
        def put(rows, v):
            ref[r, rows, :] = v
        return put

    pl.semaphore_wait(barrier, len(peers))

    def forward(q, r):
        total(q, r, into(buffers[q][2], r))
        message(q, r).start()

    order = turns(blocks, parts)
    lead = next(n for n, (q, r) in enumerate(order) if r < half)
    sent = set()
    for n, (q, r) in enumerate(order):
        pair = [r] if r >= half else [r // 2 * 2, r // 2 * 2 + 1]
        if (q, r) not in sent:
            for k in pair:
                local(q, 1, k, into(buffers[q][0], k))
                sent.add((q, k))
            across(q, r).start()
        if LAG <= n < lead + LAG:
            forward(*order[n - LAG])
    for q, r in order[min(lead, len(order) - LAG):]:
        if r:
            forward(q, r)
    for q in range(len(parts)):
        out, come, acc, got, s, t, s2, t2 = buffers[q]
        rcopy(out, come, s, t.at[0], core).wait_send()
        rest = pl.ds(1, blocks - 1)
        rcopy(acc.at[rest], got.at[rest], s2, t2.at[0], core).wait_send()

    for q in reversed(range(len(parts))):
        first, keys, _ = parts[q]

        def put(rows, v):
            if rows.start < 2 * keys:
                final[2 * first:2 * (first + keys), :] = v
            else:
                final[2 * kpd:2 * kpd + 1, :] = v

        total(q, 0, put)


def divide(kpd, final, out_hbm, cout_hbm, out_ref, cout_ref, osem):
    cf = final[2 * kpd:2 * kpd + 1, 0:kpd]
    cout_ref[...] = cf
    copies = [pltpu.make_async_copy(cout_ref, cout_hbm, osem.at[0]), pltpu.make_async_copy(out_ref, out_hbm, osem.at[1])]
    copies[0].start()
    spread = jnp.broadcast_to(jnp.maximum(cf, 1.0), (kpd, kpd))
    eye = lax.broadcasted_iota(jnp.int32, (kpd, kpd), 0) == lax.broadcasted_iota(jnp.int32, (kpd, kpd), 1)
    col = jnp.sum(jnp.where(eye, spread, 0.0), axis=1, keepdims=True)
    out_ref[:, 0:LANES] = final[pl.ds(0, kpd, stride=2), :] / col
    out_ref[:, LANES:2 * LANES] = final[pl.ds(1, kpd, stride=2), :] / col
    copies[1].start()
    for cp in copies:
        cp.wait()


def per_device(facts, row_owner, key_offset):
    n_dom, n_rep = lax.axis_size("dom"), lax.axis_size("rep")
    rows, M = facts.shape
    blocks = n_dom * n_rep // 2
    kpd = KEYS // (n_dom * n_rep)
    parts = routes(n_dom, n_rep, kpd)
    nchunks = 2

    def vm(*shape, dtype=F32):
        return pltpu.VMEM(shape, dtype)

    def dma(*shape):
        return pltpu.SemaphoreType.DMA(shape) if shape else pltpu.SemaphoreType.DMA

    I32 = jnp.int32
    pin = pltpu.with_memory_space_constraint
    hbm = pl.BlockSpec(memory_space=pltpu.HBM)
    vmem = pl.BlockSpec(memory_space=pltpu.VMEM)
    by_tile = facts.reshape(rows // 8, 8, 2, LANES).transpose(0, 2, 1, 3).reshape(2 * rows, LANES)
    square = (rows // LANES, LANES)
    ints = [row_owner.reshape(square), key_offset.reshape(square), row_owner.reshape(1, rows), key_offset.reshape(1, rows)]
    *tables, counted = pl.pallas_call(
        functools.partial(scatter, parts, n_dom, n_rep, rows),
        out_shape=[vm(2 * KEYS, LANES)] * TABLES + [vm(2 * blocks, LANES)],
        in_specs=[hbm] * 5,
        out_specs=[vmem] * (TABLES + 1),
        scratch_shapes=[
            vm(*square, dtype=I32), vm(*square, dtype=I32), vm(1, rows, dtype=I32), vm(1, rows, dtype=I32),
            vm(*square, dtype=I32), pltpu.SMEM(square, I32), vm(2 * rows, LANES),
            pltpu.SemaphoreType.DMA((4,)), pltpu.SemaphoreType.DMA, pltpu.SemaphoreType.DMA((nchunks,)),
        ],
        compiler_params=pltpu.CompilerParams(vmem_limit_bytes=8 * 1024 * 1024),
    )(*(pin(a, pltpu.HBM) for a in ints + [by_tile]))

    scratch = []
    for q, (_, keys, _) in enumerate(parts):
        scratch += [vm(blocks, 2 * keys + (q == 0), LANES)] * 4
        scratch += [dma(), dma(blocks // 2 + blocks // 4), dma(), dma(blocks // 2)]
    final = pl.pallas_call(
        functools.partial(kernel, parts, n_dom, n_rep),
        out_shape=vm(2 * kpd + 8, LANES),
        in_specs=[vmem] * (TABLES + 1),
        out_specs=vmem,
        scratch_shapes=scratch,
        compiler_params=pltpu.CompilerParams(
            collective_id=0, has_side_effects=True, vmem_limit_bytes=16 * 1024 * 1024
        ),
    )(*(pin(a, pltpu.VMEM) for a in (counted, *tables)))
    means, counts = pl.pallas_call(
        functools.partial(divide, kpd),
        out_shape=(jax.ShapeDtypeStruct((kpd, M), F32), jax.ShapeDtypeStruct((1, kpd), F32)),
        in_specs=[vmem],
        out_specs=(hbm, hbm),
        scratch_shapes=[vm(kpd, M), vm(1, kpd), pltpu.SemaphoreType.DMA((2,))],
        compiler_params=pltpu.CompilerParams(vmem_limit_bytes=4 * 1024 * 1024),
    )(pin(final, pltpu.VMEM))
    return means, counts.reshape(kpd)


def solution(mesh):
    placed = (P(("dom", "rep"), None), P(("dom", "rep"), None), P(("dom", "rep")))
    return jax.shard_map(
        per_device,
        mesh=mesh,
        in_specs=placed,
        out_specs=(P(("dom", "rep"), None), P(("dom", "rep"))),
        check_vma=False,
    )
```

```python
import functools

import jax
import jax.numpy as jnp
from jax import lax
from jax.experimental import pallas as pl
from jax.experimental.pallas import tpu as pltpu
from jax.sharding import PartitionSpec as P

KEYS = 4096
MESH = pl.DeviceIdType.MESH
F32 = jnp.float32
BF16 = jnp.bfloat16
LANES = 128
TABLES = 7
LAG = 8
TURNS = (
    31, 44, 46, 15, 63, 14, 27, 40, 60, 47, 29, 45, 43, 62, 59, 23,
    36, 55, 13, 11, 57, 30, 25, 52, 58, 10, 7, 39, 61, 9, 21, 6,
    12, 37, 26, 19, 56, 28, 5, 54, 53, 51, 8, 3, 22, 38, 42, 41,
    17, 35, 2, 50, 1, 24, 4, 33, 49, 18, 34, 20, 48, 32, 16, 0,
)


def flip(index, bits):
    at = 1
    while at <= bits:
        if bits & at:
            index = index + at * (1 - 2 * ((index // at) % 2))
        at *= 2
    return index


def log2(n):
    return n.bit_length() - 1


def routes(n_dom, n_rep, kpd):
    x, y = (0, 1), (2, 0)
    rest = [(1 << b, 0) for b in range(2, log2(n_dom))] + [(0, 1 << b) for b in range(1, log2(n_rep))]
    flat, tall = ([x, y, *rest], [y, x, *rest]), ([*rest, y, x], [*rest, x, y])
    cuts = [kpd * at // 128 // 4 * 4 for at in (0, 52, 100, 116)] + [kpd]
    ways = [flat, flat, tall, tall]
    return [(cuts[q], cuts[q + 1] - cuts[q], way) for q, way in enumerate(ways) if cuts[q] < cuts[q + 1]]


def turns(blocks, parts):
    if blocks == 16 and len(parts) == 4:
        return [divmod(turn, 16) for turn in TURNS]
    return [(q, r) for r in reversed(range(blocks)) for q in range(len(parts))]


def label(orders, n_dom, n_rep, me_d, me_r, owner, rep):
    rel_d, rel_r = owner ^ me_d, rep ^ me_r
    found = []
    for order in orders:
        r = rel_d & 1
        for bit_d, bit_r in order:
            bit = rel_d >> log2(bit_d) if bit_d else rel_r >> log2(bit_r)
            r = 2 * r + (bit & 1)
        found.append(r)
    return jnp.where((owner & 1) == 0, found[0], found[1])


def scatter(parts, n_dom, n_rep, rows, owner_hbm, offset_hbm, owner_row_hbm, offset_row_hbm, facts_hbm, *refs):
    tabs, refs = refs[:TABLES], refs[TABLES:]
    cnt_ref, owner_ref, offset_ref, owner_row, offset_row, lab_ref, at_ref, fbuf, isem, lsem, fsem = refs
    me_d, me_r = lax.axis_index("dom"), lax.axis_index("rep")
    blocks = n_dom * n_rep // 2
    kpd = KEYS // (2 * blocks)
    nchunks = fsem.shape[0]
    words = 2 * rows // nchunks
    ints = [
        pltpu.make_async_copy(src, dst, isem.at[k])
        for k, (src, dst) in enumerate(
            [(owner_hbm, owner_ref), (offset_hbm, offset_ref), (owner_row_hbm, owner_row), (offset_row_hbm, offset_row)]
        )
    ]
    loads = [
        pltpu.make_async_copy(
            facts_hbm.at[pl.ds(k * words, words)], fbuf.at[pl.ds(k * words, words)], fsem.at[k]
        )
        for k in range(nchunks)
    ]
    for ld in ints + loads:
        ld.start()

    def clear(first, last):
        @pl.loop(0, KEYS // 64)
        def _(i):
            at = pl.ds(pl.multiple_of(i * 128, 128), 128)
            for tab in tabs[first:last]:
                tab[at, :] = jnp.zeros((128, LANES), F32)

    clear(0, TABLES // 2)
    for ld in ints[:2]:
        ld.wait()
    owner, offset = owner_ref[...], offset_ref[...]
    i, base, word = offset & (kpd - 1), 0, None
    for first, keys, orders in parts:
        r = label(orders, n_dom, n_rep, me_d, me_r, owner, offset >> log2(kpd))
        at = base + 2 * (r * keys + i - first)
        word = at if word is None else jnp.where(i >= first, at, word)
        base += 4 * blocks * keys
    lab_ref[...] = word
    labels = pltpu.make_async_copy(lab_ref, at_ref, lsem)
    labels.start()
    clear(TABLES // 2, TABLES)
    for ld in ints[2:]:
        ld.wait()
    owner, offset = owner_row[...], offset_row[...]
    r = label(parts[0][2], n_dom, n_rep, me_d, me_r, owner, offset >> log2(kpd))
    i = offset & (kpd - 1)
    hot_r = jnp.where(lax.broadcasted_iota(jnp.int32, (2 * blocks, rows), 0) == r, 1.0, 0.0).astype(BF16)
    hot_i = jnp.where(lax.broadcasted_iota(jnp.int32, (LANES, rows), 0) == i, 1.0, 0.0).astype(BF16)
    cnt_ref[...] = lax.dot_general(hot_r, hot_i, (((1,), (1,)), ((), ())), preferred_element_type=F32)

    labels.wait()
    group = rows // nchunks // LANES
    for k in range(nchunks):
        loads[k].wait()

        @pl.loop(0, group)
        def _(g):
            base = pl.multiple_of((k * group + g) * 2 * LANES, 2 * LANES)
            mine = at_ref.at[k * group + g]
            for r in range(LANES):
                at = pl.ds(pl.multiple_of(mine[r], 2), 2)
                row = fbuf[pl.ds(base + 16 * (r // 8) + r % 8, 2, stride=8), :]
                tabs[r % TABLES][at, :] = tabs[r % TABLES][at, :] + row


def kernel(parts, n_dom, n_rep, cnt_ref, *refs):
    blocks = n_dom * n_rep // 2
    kpd = KEYS // (n_dom * n_rep)
    depth = log2(blocks)
    tabs, (final, *refs) = refs[:TABLES], refs[TABLES:]
    buffers = [refs[8 * q:8 * q + 8] for q in range(len(parts))]
    me_d, me_r = lax.axis_index("dom"), lax.axis_index("rep")
    c = me_d % 2
    core = (flip(me_d, 1), me_r)
    peers = [core] + [(flip(me_d, d), flip(me_r, r)) for d, r in parts[0][2][0]]
    barrier = pltpu.get_barrier_semaphore()
    for p in peers:
        pl.semaphore_signal(barrier, inc=1, device_id=p, device_id_type=MESH)

    def rcopy(src, dst, s, t, dev):
        return pltpu.make_async_remote_copy(
            src_ref=src, dst_ref=dst, send_sem=s, recv_sem=t, device_id=dev, device_id_type=MESH
        )

    half = blocks // 2

    def twins(q):
        return range(q // 2 * 2, min(q // 2 * 2 + 2, len(parts)))

    def across(q, r):
        out, come, _, _, s = buffers[q][:5]
        t = buffers[q // 2 * 2][5]
        at, n = (r, r - half // 2) if r >= half else (pl.ds(r // 2 * 2, 2), r // 2)
        return rcopy(out.at[at], come.at[at], s, t.at[n], core)

    def message(q, r):
        _, _, acc, got, _, _, s, t = buffers[q]
        step = depth - r.bit_length()
        (d0, r0), (d1, r1) = (order[step] for order in parts[q][2])
        peer = ((1 - c) * flip(me_d, d0) + c * flip(me_d, d1), (1 - c) * flip(me_r, r0) + c * flip(me_r, r1))
        return rcopy(acc.at[r], got.at[r], s, t.at[r - (half >> step)], peer)

    def arrived(q, r, n):
        _, _, acc, got, _, _, s, t = buffers[q]
        rcopy(acc.at[pl.ds(0, n)], got.at[pl.ds(0, n)], s, t.at[r], core).wait_recv()

    bases = [4 * blocks * sum(p[1] for p in parts[:q]) for q in range(len(parts))]

    def local(q, other, r, put):
        words = 2 * parts[q][1]
        at = pl.ds(bases[q] + (other * blocks + r) * words, words)
        v = tabs[0][at, :]
        for tab in tabs[1:]:
            v = v + tab[at, :]
        put(slice(0, words), v)
        if q == 0:
            put(slice(words, words + 1), cnt_ref[pl.ds(other * blocks + r, 1), :])

    paired = set()

    def total(q, r, put):
        _, come, _, got = buffers[q][:4]
        n = r - half // 2 if r >= half else r // 2
        if (q // 2, n) not in paired:
            words = sum(2 * parts[k][1] + (k == 0) for k in twins(q)) * (1 if r >= half else 2)
            some = tabs[0].at[pl.ds(0, words)]
            rcopy(some, some, buffers[q][4], buffers[q // 2 * 2][5].at[n], core).wait_recv()
            paired.add((q // 2, n))
        come_from = [come.at[r]]
        step = depth - r.bit_length()
        if step:
            arrived(q, r, step)
        for k in range(step):
            come_from.append(got.at[r + (half >> k)])

        def add(rows, v):
            for ref in come_from:
                v = v + ref[rows, :]
            put(rows, v)

        local(q, 0, r, add)

    def into(ref, r):
        def put(rows, v):
            ref[r, rows, :] = v
        return put

    pl.semaphore_wait(barrier, len(peers))

    def forward(q, r):
        total(q, r, into(buffers[q][2], r))
        message(q, r).start()

    order = turns(blocks, parts)
    lead = next(n for n, (q, r) in enumerate(order) if r < half)
    sent = set()
    for n, (q, r) in enumerate(order):
        pair = [r] if r >= half else [r // 2 * 2, r // 2 * 2 + 1]
        if (q, r) not in sent:
            for j in twins(q):
                for k in pair:
                    local(j, 1, k, into(buffers[j][0], k))
                    sent.add((j, k))
                across(j, r).start()
        if LAG <= n < lead + LAG:
            forward(*order[n - LAG])
    for q, r in order[min(lead, len(order) - LAG):]:
        if r:
            forward(q, r)
    for q in range(len(parts)):
        out, come, acc, got, s, t, s2, t2 = buffers[q]
        rcopy(out, come, s, t2.at[0], core).wait_send()
        rest = pl.ds(1, blocks - 1)
        rcopy(acc.at[rest], got.at[rest], s2, t2.at[0], core).wait_send()

    for q in reversed(range(len(parts))):
        first, keys, _ = parts[q]

        def put(rows, v):
            if rows.start < 2 * keys:
                final[2 * first:2 * (first + keys), :] = v
            else:
                final[2 * kpd:2 * kpd + 1, :] = v

        total(q, 0, put)


def divide(kpd, final, out_hbm, cout_hbm, out_ref, cout_ref, osem):
    cf = final[2 * kpd:2 * kpd + 1, 0:kpd]
    cout_ref[...] = cf
    copies = [pltpu.make_async_copy(cout_ref, cout_hbm, osem.at[0]), pltpu.make_async_copy(out_ref, out_hbm, osem.at[1])]
    copies[0].start()
    spread = jnp.broadcast_to(jnp.maximum(cf, 1.0), (kpd, kpd))
    eye = lax.broadcasted_iota(jnp.int32, (kpd, kpd), 0) == lax.broadcasted_iota(jnp.int32, (kpd, kpd), 1)
    col = jnp.sum(jnp.where(eye, spread, 0.0), axis=1, keepdims=True)
    out_ref[:, 0:LANES] = final[pl.ds(0, kpd, stride=2), :] / col
    out_ref[:, LANES:2 * LANES] = final[pl.ds(1, kpd, stride=2), :] / col
    copies[1].start()
    for cp in copies:
        cp.wait()


def per_device(facts, row_owner, key_offset):
    n_dom, n_rep = lax.axis_size("dom"), lax.axis_size("rep")
    rows, M = facts.shape
    blocks = n_dom * n_rep // 2
    kpd = KEYS // (n_dom * n_rep)
    parts = routes(n_dom, n_rep, kpd)
    nchunks = 2

    def vm(*shape, dtype=F32):
        return pltpu.VMEM(shape, dtype)

    def dma(*shape):
        return pltpu.SemaphoreType.DMA(shape) if shape else pltpu.SemaphoreType.DMA

    I32 = jnp.int32
    pin = pltpu.with_memory_space_constraint
    hbm = pl.BlockSpec(memory_space=pltpu.HBM)
    vmem = pl.BlockSpec(memory_space=pltpu.VMEM)
    by_tile = facts.reshape(rows // 8, 8, 2, LANES).transpose(0, 2, 1, 3).reshape(2 * rows, LANES)
    square = (rows // LANES, LANES)
    ints = [row_owner.reshape(square), key_offset.reshape(square), row_owner.reshape(1, rows), key_offset.reshape(1, rows)]
    *tables, counted = pl.pallas_call(
        functools.partial(scatter, parts, n_dom, n_rep, rows),
        out_shape=[vm(2 * KEYS, LANES)] * TABLES + [vm(2 * blocks, LANES)],
        in_specs=[hbm] * 5,
        out_specs=[vmem] * (TABLES + 1),
        scratch_shapes=[
            vm(*square, dtype=I32), vm(*square, dtype=I32), vm(1, rows, dtype=I32), vm(1, rows, dtype=I32),
            vm(*square, dtype=I32), pltpu.SMEM(square, I32), vm(2 * rows, LANES),
            pltpu.SemaphoreType.DMA((4,)), pltpu.SemaphoreType.DMA, pltpu.SemaphoreType.DMA((nchunks,)),
        ],
        compiler_params=pltpu.CompilerParams(vmem_limit_bytes=8 * 1024 * 1024),
    )(*(pin(a, pltpu.HBM) for a in ints + [by_tile]))

    scratch = []
    for q, (_, keys, _) in enumerate(parts):
        scratch += [vm(blocks, 2 * keys + (q == 0), LANES)] * 4
        scratch += [dma(), dma(blocks // 2 + blocks // 4) if q % 2 == 0 else dma(), dma(), dma(blocks // 2)]
    final = pl.pallas_call(
        functools.partial(kernel, parts, n_dom, n_rep),
        out_shape=vm(2 * kpd + 8, LANES),
        in_specs=[vmem] * (TABLES + 1),
        out_specs=vmem,
        scratch_shapes=scratch,
        compiler_params=pltpu.CompilerParams(
            collective_id=0, has_side_effects=True, vmem_limit_bytes=16 * 1024 * 1024
        ),
    )(*(pin(a, pltpu.VMEM) for a in (counted, *tables)))
    means, counts = pl.pallas_call(
        functools.partial(divide, kpd),
        out_shape=(jax.ShapeDtypeStruct((kpd, M), F32), jax.ShapeDtypeStruct((1, kpd), F32)),
        in_specs=[vmem],
        out_specs=(hbm, hbm),
        scratch_shapes=[vm(kpd, M), vm(1, kpd), pltpu.SemaphoreType.DMA((2,))],
        compiler_params=pltpu.CompilerParams(vmem_limit_bytes=4 * 1024 * 1024),
    )(pin(final, pltpu.VMEM))
    return means, counts.reshape(kpd)


def solution(mesh):
    placed = (P(("dom", "rep"), None), P(("dom", "rep"), None), P(("dom", "rep")))
    return jax.shard_map(
        per_device,
        mesh=mesh,
        in_specs=placed,
        out_specs=(P(("dom", "rep"), None), P(("dom", "rep"))),
        check_vma=False,
    )
```
